128 devices in a mesh: data: 1, seq: 64 (over z, y, x), dap: 2 (over core).
Axes of the slice: x: 4, y: 4, z: 4, core: 2. Of those that a mesh axis runs over, the one named last changes fastest.
Arguments:
- msa_act: bfloat16 [2048, 512, 64], P(('data', 'seq'), 'dap')
- msa_mask: int32 [2048, 512], P('data')
- pair_act: float32 [512, 512, 128], P(('data', 'dap'))
- ln_gamma: bfloat16 [64], replicated
- ln_beta: bfloat16 [64], replicated
- w_left: bfloat16 [64, 32], replicated
- b_left: bfloat16 [32], replicated
- w_right: bfloat16 [64, 32], replicated
- b_right: bfloat16 [32], replicated
- w_out: bfloat16 [1024, 128], replicated
- b_out: bfloat16 [128], replicated
Outputs:
- output 1: float32 [512, 512, 128], P(('data', 'dap'))
- output 2: bfloat16 [2048, 512, 64], P(('data', 'seq', 'dap'))
All inputs are finite; a program needn't handle non-finite values.
Results may differ from the reference program's by a relative error of at most 0.0127676.
Values are sent between devices in bfloat16 or wider.
A program may use at most 1 GiB of HBM per device.

```python
import math
import jax
import jax.numpy as jnp
from jax import lax

S = 2048
N = 512
CM = 64
CH = 32
CZ = 128
ROW_BLOCK = math.gcd(N, 16)


def setup_inputs(seed: int = 0, part: int = 0) -> dict:
    root_key = jax.random.key(seed)
    shared_root, part_root = jax.random.split(root_key)
    part_key = jax.random.fold_in(part_root, part)
    part_keys = jax.random.split(part_key, 5)
    weight_keys = jax.random.split(shared_root, 8)
    bias_scale = 0.5 * S ** -0.25
    msa_act = jax.random.normal(part_keys[0], (S, N, CM), jnp.float32).astype(jnp.bfloat16)
    col_level = jax.random.randint(part_keys[1], (N,), 8, 16)
    row_shift = jax.random.randint(part_keys[2], (S,), -2, 3)
    draw_mask = jax.random.randint(part_keys[3], (S, N), 0, 16)
    kept_mask = (draw_mask < col_level[None, :] + row_shift[:, None]).astype(jnp.int32)
    first_row = (jnp.arange(S) == 0).astype(jnp.int32)[:, None]
    msa_mask = jnp.maximum(kept_mask, first_row)
    pair_act = 0.5 * jax.random.normal(part_keys[4], (N, N, CZ), jnp.float32)
    ln_gamma = (1.0 + 0.3 * jax.random.normal(weight_keys[0], (CM,), jnp.float32)).astype(jnp.bfloat16)
    ln_beta = (bias_scale * jax.random.normal(weight_keys[1], (CM,), jnp.float32)).astype(jnp.bfloat16)
    w_left = (jax.random.normal(weight_keys[2], (CM, CH), jnp.float32) * CM ** -0.5).astype(jnp.bfloat16)
    b_left = (bias_scale * jax.random.normal(weight_keys[3], (CH,), jnp.float32)).astype(jnp.bfloat16)
    w_right = (jax.random.normal(weight_keys[4], (CM, CH), jnp.float32) * CM ** -0.5).astype(jnp.bfloat16)
    b_right = (bias_scale * jax.random.normal(weight_keys[5], (CH,), jnp.float32)).astype(jnp.bfloat16)
    w_out = (jax.random.normal(weight_keys[6], (CH * CH, CZ), jnp.float32) * (0.5 * math.sqrt(S) / CH)).astype(jnp.bfloat16)
    b_out = (0.25 * S * jax.random.normal(weight_keys[7], (CZ,), jnp.float32)).astype(jnp.bfloat16)
    return {'msa_act': msa_act, 'msa_mask': msa_mask, 'pair_act': pair_act, 'ln_gamma': ln_gamma, 'ln_beta': ln_beta, 'w_left': w_left, 'b_left': b_left, 'w_right': w_right, 'b_right': b_right, 'w_out': w_out, 'b_out': b_out}


def layer_norm(msa_act, ln_gamma, ln_beta):
    act_f32 = msa_act.astype(jnp.float32)
    mean_val = jnp.mean(act_f32, axis=-1, keepdims=True)
    centered = act_f32 - mean_val
    var_val = jnp.mean(centered * centered, axis=-1, keepdims=True)
    normed = centered * lax.rsqrt(var_val + 1e-5)
    return (normed * ln_gamma.astype(jnp.float32) + ln_beta.astype(jnp.float32)).astype(jnp.bfloat16)


def project(normed, weight, bias_vec, mask_f32):
    flat_act = normed.reshape(-1, normed.shape[-1])
    out_f32 = jnp.dot(flat_act, weight, preferred_element_type=jnp.float32) + bias_vec.astype(jnp.float32)
    return (out_f32.reshape(normed.shape[:-1] + (weight.shape[1],)) * mask_f32[:, :, None]).astype(jnp.bfloat16)


def reference(msa_act, msa_mask, pair_act, ln_gamma, ln_beta, w_left, b_left, w_right, b_right, w_out, b_out):
    normed = layer_norm(msa_act, ln_gamma, ln_beta)
    mask_f32 = msa_mask.astype(jnp.float32)
    left_proj = project(normed, w_left, b_left, mask_f32)
    right_proj = project(normed, w_right, b_right, mask_f32)
    right_f32 = right_proj.astype(jnp.float32)
    w_out3 = w_out.astype(jnp.float32).reshape(CH, CH, CZ)
    left_blocks = jnp.moveaxis(left_proj.astype(jnp.float32).reshape(S, N // ROW_BLOCK, ROW_BLOCK, CH), 1, 0)

    def row_block(left_blk):
        outer_blk = jnp.einsum('sic,sjd->icjd', left_blk, right_f32).astype(jnp.bfloat16)
        return jnp.einsum('icjd,cde->ije', outer_blk.astype(jnp.float32), w_out3)

    proj_sum = lax.map(row_block, left_blocks).reshape(N, N, CZ)
    pair_count = jnp.dot(mask_f32.T, mask_f32)
    pair_out = pair_act + (proj_sum + b_out.astype(jnp.float32)) / (1e-3 + pair_count)[:, :, None]
    return pair_out, msa_act
```

```python
import functools

import jax
import jax.numpy as jnp
from jax import lax
from jax.experimental import pallas as pl
from jax.experimental.pallas import tpu as pltpu
from jax.sharding import PartitionSpec as P

CHUNKS = 4


def layer_norm(value, ln_gamma, ln_beta):
    act_f32 = value.astype(jnp.float32)
    mean_val = jnp.mean(act_f32, axis=-1, keepdims=True)
    centered = act_f32 - mean_val
    var_val = jnp.mean(centered * centered, axis=-1, keepdims=True)
    normed = centered * lax.rsqrt(var_val + 1e-5)
    return (normed * ln_gamma.astype(jnp.float32) + ln_beta.astype(jnp.float32)).astype(jnp.bfloat16)


def project(normed, weight, bias_vec, mask_f32):
    out_f32 = jnp.einsum('sic,cd->sid', normed, weight, preferred_element_type=jnp.float32)
    out_f32 = out_f32 + bias_vec.astype(jnp.float32)
    return (out_f32 * mask_f32[:, :, None]).astype(jnp.bfloat16)


def update_kernel(rows, chunk, z_ref, g_ref, inv_ref, b_ref, *rest):
    out_ref = rest[-1]
    blk = pl.program_id(0) * 16 + pl.program_id(1) * 4 + chunk
    shift = lax.rem(blk * rows, 128)
    inv = pltpu.roll(inv_ref[...], lax.rem(128 - shift, 128), 1)
    bias = b_ref[...]
    for r in range(rows):
        col = inv[:, r:r + 1]
        for h in range(2):
            for y in range(4):
                j0 = h * 256 + y * 64
                seg = g_ref[0, y, 0, r, h].astype(jnp.float32)
                out_ref[r, j0:j0 + 64, :] = z_ref[r, j0:j0 + 64, :] + (seg + bias) * col[j0:j0 + 64]


def update(chunk, n_chunks, pair_rows, gathered, inv_t, bias, prev):
    rows = 16 // n_chunks
    g = gathered.reshape(4, 4, 4, rows, 2, 64, 128)
    row_map = lambda zi, xi: (zi * 16 + xi * 4 + chunk, 0, 0) if n_chunks == 4 else None
    in_specs = [
        pl.BlockSpec((rows, 512, 128), row_map),
        pl.BlockSpec((1, 4, 1, rows, 2, 64, 128), lambda zi, xi: (zi, 0, xi, 0, 0, 0, 0)),
        pl.BlockSpec((512, 128), lambda zi, xi: (0, (zi * 64 + xi * 16 + chunk * rows) // 128)),
        pl.BlockSpec((1, 128), lambda zi, xi: (0, 0)),
    ]
    args = [pair_rows, g, inv_t, bias]
    aliases = {}
    if prev is not None:
        in_specs.append(pl.BlockSpec(memory_space=pl.ANY))
        args.append(prev)
        aliases = {4: 0}
    return pl.pallas_call(
        functools.partial(update_kernel, rows, chunk),
        grid=(4, 4),
        in_specs=in_specs,
        out_specs=pl.BlockSpec((rows, 512, 128), row_map),
        out_shape=jax.ShapeDtypeStruct(pair_rows.shape, jnp.float32),
        input_output_aliases=aliases,
        cost_estimate=pl.CostEstimate(flops=30_000_000_000, bytes_accessed=40_000_000, transcendentals=0),
        name='update_%d' % chunk,
    )(*args)


def solution(mesh):
    rep = P()
    in_specs = (P(('data', 'seq'), 'dap', None), P('data', None), P(('data', 'dap'), None, None)) + (rep,) * 8
    out_specs = (P(('data', 'dap'), None, None), P(('data', 'seq', 'dap'), None, None))
    rng = range(4)
    zgroups = [[z * 16 + y * 4 + x for z in rng] for y in rng for x in rng]
    ygroups = [[z * 16 + y * 4 + x for y in rng] for z in rng for x in rng]
    xgroups = [[z * 16 + y * 4 + x for x in rng] for z in rng for y in rng]

    def local_fn(msa, mask, pair_rows, ln_gamma, ln_beta, w_left, b_left, w_right, b_right, w_out, b_out):
        seq_idx = lax.axis_index('seq')
        dap_idx = lax.axis_index('dap')
        msa_out = lax.all_to_all(msa, 'dap', 0, 1, tiled=True)
        mask_seq = lax.dynamic_slice(mask, (seq_idx * 32, dap_idx * 256), (32, 256)).astype(jnp.float32)
        normed = layer_norm(msa, ln_gamma, ln_beta)
        left = project(normed, w_left, b_left, mask_seq)
        right = project(normed, w_right, b_right, mask_seq)
        left = lax.all_to_all(left, 'seq', 1, 0, axis_index_groups=zgroups, tiled=True)
        left = lax.all_gather(left, 'seq', axis=0, axis_index_groups=ygroups, tiled=True)
        right = lax.all_to_all(right, 'seq', 1, 0, axis_index_groups=ygroups, tiled=True)
        right = lax.all_gather(right, 'seq', axis=0, axis_index_groups=zgroups, tiled=True)
        right = lax.all_gather(right, 'dap', axis=1, tiled=True)
        right = right.reshape(4, 4, 32, 128, 32).transpose(1, 0, 2, 3, 4).reshape(512, 128, 32)
        w3 = w_out.reshape(32, 32, 128)
        outer = jnp.einsum('sic,sjd->icjd', left, right, preferred_element_type=jnp.float32).astype(jnp.bfloat16)
        partial = jnp.einsum('icjd,cde->ije', outer, w3, preferred_element_type=jnp.float32).astype(jnp.bfloat16)
        parts = lax.all_to_all(partial.reshape(4, 16, 128, 128), 'seq', 0, 0, axis_index_groups=xgroups, tiled=True)
        total = jnp.sum(parts.astype(jnp.float32), axis=0).astype(jnp.bfloat16)

        mask_bf16 = mask.astype(jnp.bfloat16)
        mask_rows = lax.dynamic_slice_in_dim(mask_bf16, dap_idx * 256, 256, axis=1)
        count_t = jnp.einsum('sj,si->ji', mask_bf16, mask_rows, preferred_element_type=jnp.float32)
        inv_t = 1.0 / (1e-3 + count_t)
        bias = b_out.astype(jnp.float32).reshape(1, 128)

        rows = 16 // CHUNKS
        gathered = [lax.all_gather(total[k * rows:(k + 1) * rows], 'seq', axis=0) for k in range(CHUNKS)]
        out = None
        for k in range(CHUNKS):
            out = update(k, CHUNKS, pair_rows, gathered[k], inv_t, bias, out)
        return out, msa_out

    return jax.shard_map(local_fn, mesh=mesh, in_specs=in_specs, out_specs=out_specs, check_vma=False)
```

```python
import jax
import jax.numpy as jnp
from jax import lax
from jax.experimental import pallas as pl
from jax.experimental.pallas import tpu as pltpu
from jax.sharding import PartitionSpec as P


def layer_norm(value, ln_gamma, ln_beta):
    act_f32 = value.astype(jnp.float32)
    mean_val = jnp.mean(act_f32, axis=-1, keepdims=True)
    centered = act_f32 - mean_val
    var_val = jnp.mean(centered * centered, axis=-1, keepdims=True)
    normed = centered * lax.rsqrt(var_val + 1e-5)
    return (normed * ln_gamma.astype(jnp.float32) + ln_beta.astype(jnp.float32)).astype(jnp.bfloat16)


def project(normed, weight, bias_vec, mask_f32):
    out_f32 = jnp.einsum('sic,cd->sid', normed, weight, preferred_element_type=jnp.float32)
    out_f32 = out_f32 + bias_vec.astype(jnp.float32)
    return (out_f32 * mask_f32[:, :, None]).astype(jnp.bfloat16)


AXES = ((2, 1, 0), (1, 0, 2), (0, 2, 1))
SPLIT = (((0, 6), (6, 5)), ((11, 6), (17, 5)), ((22, 5), (27, 5)))


def gather_kernel(t_ref, g_ref, send_sem, recv_sem, own_sem):
    seq = lax.axis_index('seq')
    me = (seq // 16, lax.rem(seq // 4, 4), lax.rem(seq, 4))
    strides = (16, 4, 1)

    def peer(axis, step):
        pos = lax.rem(me[axis] + step + 4, 4)
        return {'seq': seq + (pos - me[axis]) * strides[axis]}

    barrier = pltpu.get_barrier_semaphore()
    for axis in range(3):
        for step in (1, -1):
            pl.semaphore_signal(barrier, inc=1, device_id=peer(axis, step), device_id_type=pl.DeviceIdType.MESH)
    pl.semaphore_wait(barrier, 6)

    def block(part, phase, shift, u0, n):
        idx = [pl.ds(me[a], 1) for a in range(3)]
        for done in range(phase):
            idx[AXES[part][done]] = pl.ds(0, 4)
        axis = AXES[part][phase]
        idx[axis] = pl.ds(lax.rem(me[axis] + shift + 4, 4), 1)
        return g_ref.at[idx[0], idx[1], idx[2], pl.ds(u0, n)]

    def message(c, part, phase, kind):
        u0, n = SPLIT[part][c]
        lo = (n + 1) // 2 if (part + c) % 2 == 0 else n // 2
        if kind == 2:
            n = lo
        elif kind == 3:
            u0, n = u0 + lo, n - lo
        return u0, n

    def copy(c, part, phase, kind, shift):
        u0, n = message(c, part, phase, kind)
        ref = block(part, phase, shift, u0, n)
        src = ref
        if phase == 0 and shift == 0:
            src = t_ref.at[:, :, :, pl.ds(u0, n)]
        return pltpu.make_async_remote_copy(
            src_ref=src, dst_ref=ref, send_sem=send_sem.at[c, part, phase, kind],
            recv_sem=recv_sem.at[c, part, phase, kind],
            device_id=peer(AXES[part][phase], 1 if kind % 2 == 0 else -1),
            device_id_type=pl.DeviceIdType.MESH)

    sent_shift = (0, 0, -1, 1)
    got_shift = (-1, 1, -2, 2)
    own = pltpu.make_async_copy(t_ref, g_ref.at[pl.ds(me[0], 1), pl.ds(me[1], 1), pl.ds(me[2], 1)], own_sem)
    order = [(c, p) for c in range(2) for p in range(3)]
    for c, p in order:
        copy(c, p, 0, 0, 0).start()
        copy(c, p, 0, 1, 0).start()
    own.start()
    own.wait()
    for phase in range(3):
        for c, p in order:
            for kind in (0, 1):
                copy(c, p, phase, kind, got_shift[kind]).wait_recv()
                copy(c, p, phase, kind + 2, sent_shift[kind + 2]).start()
        for c, p in order:
            for kind in (2, 3):
                copy(c, p, phase, kind, got_shift[kind]).wait_recv()
            if phase < 2:
                copy(c, p, phase + 1, 0, 0).start()
                copy(c, p, phase + 1, 1, 0).start()
    for phase in range(3):
        for c, p in order:
            for kind in range(4):
                copy(c, p, phase, kind, sent_shift[kind]).wait_send()


def gather(tile):
    return pl.pallas_call(
        gather_kernel,
        in_specs=[pl.BlockSpec(memory_space=pltpu.VMEM)],
        out_specs=pl.BlockSpec(memory_space=pl.ANY),
        out_shape=jax.ShapeDtypeStruct((4, 4, 4, 32, 64, 128), jnp.bfloat16),
        scratch_shapes=[pltpu.SemaphoreType.DMA((2, 3, 3, 4)), pltpu.SemaphoreType.DMA((2, 3, 3, 4)), pltpu.SemaphoreType.DMA],
        compiler_params=pltpu.CompilerParams(collective_id=1, has_side_effects=True),
        name='gather_tiles',
    )(tile.reshape(1, 1, 1, 32, 64, 128))


ROWS = 8


def update_kernel(z_ref, g_ref, inv_ref, b_ref, out_ref):
    blk = (pl.program_id(0) * 4 + pl.program_id(1)) * (16 // ROWS) + pl.program_id(2)
    shift = lax.rem(blk * ROWS, 128)
    inv = pltpu.roll(inv_ref[...], lax.rem(128 - shift, 128), 1)
    bias = b_ref[...]
    for r in range(ROWS):
        col = inv[:, r:r + 1]
        for h in range(2):
            for y in range(4):
                j0 = h * 256 + y * 64
                seg = g_ref[0, y, 0, 2 * r + h].astype(jnp.float32)
                out_ref[r, j0:j0 + 64, :] = z_ref[r, j0:j0 + 64, :] + (seg + bias) * col[j0:j0 + 64]


def update(pair_rows, gathered, inv_t, bias):
    nb = 16 // ROWS
    row_map = lambda zi, xi, ri: ((zi * 4 + xi) * nb + ri, 0, 0)
    return pl.pallas_call(
        update_kernel,
        grid=(4, 4, nb),
        in_specs=[
            pl.BlockSpec((ROWS, 512, 128), row_map),
            pl.BlockSpec((1, 4, 1, 2 * ROWS, 64, 128), lambda zi, xi, ri: (zi, 0, xi, ri, 0, 0)),
            pl.BlockSpec((512, 128), lambda zi, xi, ri: (0, zi // 2)),
            pl.BlockSpec((1, 128), lambda zi, xi, ri: (0, 0)),
        ],
        out_specs=pl.BlockSpec((ROWS, 512, 128), row_map),
        out_shape=jax.ShapeDtypeStruct(pair_rows.shape, jnp.float32),
        cost_estimate=pl.CostEstimate(flops=30_000_000_000, bytes_accessed=160_000_000, transcendentals=0),
        name='update',
    )(pair_rows, gathered, inv_t, bias)


def solution(mesh):
    rep = P()
    in_specs = (P(('data', 'seq'), 'dap', None), P('data', None), P(('data', 'dap'), None, None)) + (rep,) * 8
    out_specs = (P(('data', 'dap'), None, None), P(('data', 'seq', 'dap'), None, None))
    rng = range(4)
    zgroups = [[z * 16 + y * 4 + x for z in rng] for y in rng for x in rng]
    ygroups = [[z * 16 + y * 4 + x for y in rng] for z in rng for x in rng]
    xgroups = [[z * 16 + y * 4 + x for x in rng] for z in rng for y in rng]

    def local_fn(msa, mask, pair_rows, ln_gamma, ln_beta, w_left, b_left, w_right, b_right, w_out, b_out):
        seq_idx = lax.axis_index('seq')
        dap_idx = lax.axis_index('dap')
        msa_out = lax.all_to_all(msa, 'dap', 0, 1, tiled=True)
        mask_seq = lax.dynamic_slice(mask, (seq_idx * 32, dap_idx * 256), (32, 256)).astype(jnp.float32)
        normed = layer_norm(msa, ln_gamma, ln_beta)
        left = project(normed, w_left, b_left, mask_seq)
        right = project(normed, w_right, b_right, mask_seq)
        left = lax.all_to_all(left, 'seq', 1, 0, axis_index_groups=zgroups, tiled=True)
        left = lax.all_gather(left, 'seq', axis=0, axis_index_groups=ygroups, tiled=True)
        right = lax.all_to_all(right, 'seq', 1, 0, axis_index_groups=ygroups, tiled=True)
        right = lax.all_gather(right, 'seq', axis=0, axis_index_groups=zgroups, tiled=True)
        right = lax.all_gather(right, 'dap', axis=1, tiled=True)
        right = right.reshape(4, 4, 32, 128, 32).transpose(1, 0, 2, 3, 4).reshape(512, 128, 32)
        w3 = w_out.reshape(32, 32, 128)
        outer = jnp.einsum('sic,sjd->icjd', left, right, preferred_element_type=jnp.float32).astype(jnp.bfloat16)
        partial = jnp.einsum('icjd,cde->ije', outer, w3, preferred_element_type=jnp.float32).astype(jnp.bfloat16)
        parts = lax.all_to_all(partial.reshape(4, 16, 128, 128), 'seq', 0, 0, axis_index_groups=xgroups, tiled=True)
        total = jnp.sum(parts.astype(jnp.float32), axis=0).astype(jnp.bfloat16)

        mask_bf16 = mask.astype(jnp.bfloat16)
        mask_rows = lax.dynamic_slice_in_dim(mask_bf16, dap_idx * 256, 256, axis=1)
        count_t = jnp.einsum('sj,si->ji', mask_bf16, mask_rows, preferred_element_type=jnp.float32)
        inv_t = 1.0 / (1e-3 + count_t)
        bias = b_out.astype(jnp.float32).reshape(1, 128)

        out = update(pair_rows, gather(total), inv_t, bias)
        return out, msa_out

    return jax.shard_map(local_fn, mesh=mesh, in_specs=in_specs, out_specs=out_specs, check_vma=False)
```

```python
import jax
import jax.numpy as jnp
from jax import lax
from jax.experimental import pallas as pl
from jax.experimental.pallas import tpu as pltpu
from jax.sharding import PartitionSpec as P


STRIDE = 72


def project_kernel(m_ref, mask_ref, gamma_ref, beta_ref, w_ref, bias_ref, a_ref, b_ref, scr):
    gamma, beta, bias = gamma_ref[...], beta_ref[...], bias_ref[...]
    w = w_ref[...]
    for s in range(32):
        x = m_ref[s].astype(jnp.float32)
        cen = x - jnp.mean(x, axis=0, keepdims=True)
        var = jnp.mean(cen * cen, axis=0, keepdims=True)
        normed = (cen * lax.rsqrt(var + 1e-5) * gamma + beta).astype(jnp.bfloat16)
        out = (jnp.dot(w, normed, preferred_element_type=jnp.float32) + bias) * mask_ref[s:s + 1, :]
        for t in range(2):
            scr[t, s * STRIDE:s * STRIDE + 64, :] = out[:, t * 128:t * 128 + 128]
    low = lax.broadcasted_iota(jnp.int32, (32, 128), 1) < 64
    for t in range(2):
        for c in range(16):
            lo = scr[t, pl.ds(c, 32, stride=STRIDE), :]
            hi = scr[t, pl.ds(16 + c, 32, stride=STRIDE), :]
            a_ref[2 * t, c] = jnp.where(low, lo, pltpu.roll(hi, 64, 1)).astype(jnp.bfloat16)
            a_ref[2 * t + 1, c] = jnp.where(low, pltpu.roll(lo, 64, 1), hi).astype(jnp.bfloat16)
        for d in range(32):
            b_ref[d // 16, t, d % 16] = scr[t, pl.ds(32 + d, 32, stride=STRIDE), :].astype(jnp.bfloat16)


def project(msa_t, mask_f32, gamma, beta, w_cat, bias_cat):
    return pl.pallas_call(
        project_kernel,
        out_shape=(jax.ShapeDtypeStruct((4, 16, 32, 128), jnp.bfloat16), jax.ShapeDtypeStruct((2, 2, 16, 32, 128), jnp.bfloat16)),
        scratch_shapes=[pltpu.VMEM((2, 32 * STRIDE, 128), jnp.float32)],
        name='project',
    )(msa_t, mask_f32, gamma, beta, w_cat, bias_cat)


MESH = pl.DeviceIdType.MESH


def exchange_kernel(a_in, b_in, a_out, b_out, b_mid, dap_sem, loc_sem, aa_send, aa_recv, bb_send, bb_recv, ag_send, ag_recv, bg_send, bg_recv, sib_send, sib_recv):
    seq = lax.axis_index('seq')
    core = lax.axis_index('dap')
    z, y = seq // 16, lax.rem(seq // 4, 4)

    def zpos(step):
        return lax.rem(z + step + 4, 4)

    def ypos(step):
        return lax.rem(y + step + 4, 4)

    def zpeer(step):
        return {'seq': seq + (zpos(step) - z) * 16}

    def ypeer(step):
        return {'seq': seq + (ypos(step) - y) * 4}

    sibling = {'dap': 1 - core}
    barrier = pltpu.get_barrier_semaphore()
    for peer in [zpeer(i) for i in (1, 2, 3)] + [ypeer(i) for i in (1, 2, 3)] + [sibling]:
        pl.semaphore_signal(barrier, inc=1, device_id=peer, device_id_type=MESH)
    pl.semaphore_wait(barrier, 7)

    def remote(src, dst, ssem, rsem, peer):
        return pltpu.make_async_remote_copy(src_ref=src, dst_ref=dst, send_sem=ssem, recv_sem=rsem, device_id=peer, device_id_type=MESH)

    to_sib = remote(b_in.at[1 - core], b_mid.at[pl.ds(2 * core, 2)], dap_sem.at[0], dap_sem.at[1], sibling)
    to_sib.start()
    mine_b = pltpu.make_async_copy(b_in.at[core], b_mid.at[pl.ds(2 * core, 2)], loc_sem.at[0])
    mine_b.start()
    mine_a = pltpu.make_async_copy(a_in.at[z], a_out.at[:, y, z], loc_sem.at[1])
    mine_a.start()

    def a_scatter(shift):
        return remote(a_in.at[zpos(shift)], a_out.at[:, y, z], aa_send.at[shift], aa_recv.at[shift], zpeer(shift))

    def a_scattered(shift):
        ref = a_out.at[:, y, zpos(-shift)]
        return remote(ref, ref, aa_send.at[shift], aa_recv.at[shift], zpeer(shift))

    def b_scatter(shift):
        return remote(b_mid.at[ypos(shift)], b_out.at[core, :, y, z], bb_send.at[shift], bb_recv.at[shift], ypeer(shift))

    def b_scattered(shift):
        ref = b_out.at[core, :, ypos(-shift), z]
        return remote(ref, ref, bb_send.at[shift], bb_recv.at[shift], ypeer(shift))

    for shift in (1, 3, 2):
        a_scatter(shift).start()
    got = b_mid.at[pl.ds(2 * (1 - core), 2)]
    remote(got, got, dap_sem.at[0], dap_sem.at[1], sibling).wait_recv()
    mine_b.wait()
    for shift in (1, 3, 2):
        b_scatter(shift).start()
    b_out[core, :, y, z] = b_mid[y]

    half = ((0, 16), (0, 16), (0, 8), (8, 8))
    shifts = (0, 0, -1, 1)
    landed = (-1, 1, -2, 2)

    def a_gather(kind, shift):
        c0, n = half[kind]
        ref = a_out.at[pl.ds(c0, n), ypos(shift)]
        return remote(ref, ref, ag_send.at[kind], ag_recv.at[kind], ypeer(1 if kind % 2 == 0 else -1))

    def b_gather(kind, shift):
        c0, n = half[kind]
        ref = b_out.at[core, pl.ds(c0, n), :, zpos(shift)]
        return remote(ref, ref, bg_send.at[kind], bg_recv.at[kind], zpeer(1 if kind % 2 == 0 else -1))

    def share(slot, which, shift, kind):
        c0, n = half[kind]
        ref = b_out.at[which, pl.ds(c0, n), :, zpos(shift)]
        return remote(ref, ref, sib_send.at[slot], sib_recv.at[slot], sibling)

    shared = ((0, 0), (-1, 0), (1, 0), (-2, 2), (2, 3))
    for shift in (1, 3, 2):
        a_scattered(shift).wait_recv()
    mine_a.wait()
    a_gather(0, 0).start()
    a_gather(1, 0).start()
    for shift in (1, 3, 2):
        b_scattered(shift).wait_recv()
    b_gather(0, 0).start()
    b_gather(1, 0).start()
    share(0, core, *shared[0]).start()
    for kind in (0, 1):
        a_gather(kind, landed[kind]).wait_recv()
        a_gather(kind + 2, shifts[kind + 2]).start()
        b_gather(kind, landed[kind]).wait_recv()
        b_gather(kind + 2, shifts[kind + 2]).start()
        share(kind + 1, core, *shared[kind + 1]).start()
    for kind in (2, 3):
        b_gather(kind, landed[kind]).wait_recv()
        share(kind + 1, core, *shared[kind + 1]).start()
    for kind in (2, 3):
        a_gather(kind, landed[kind]).wait_recv()
    for slot in range(5):
        share(slot, 1 - core, *shared[slot]).wait_recv()
    to_sib.wait_send()
    for shift in (1, 3, 2):
        a_scatter(shift).wait_send()
        b_scatter(shift).wait_send()
    for kind in range(4):
        a_gather(kind, shifts[kind]).wait_send()
        b_gather(kind, shifts[kind]).wait_send()
    for slot in range(5):
        share(slot, core, *shared[slot]).wait_send()


def exchange(a_loc, b_loc):
    dma = pltpu.SemaphoreType.DMA
    return pl.pallas_call(
        exchange_kernel,
        in_specs=[pl.BlockSpec(memory_space=pl.ANY)] * 2,
        out_specs=(pl.BlockSpec(memory_space=pltpu.VMEM),) * 2,
        out_shape=(jax.ShapeDtypeStruct((16, 4, 4, 32, 128), jnp.bfloat16), jax.ShapeDtypeStruct((2, 16, 4, 4, 32, 128), jnp.bfloat16)),
        scratch_shapes=[pltpu.VMEM((4, 16, 32, 128), jnp.bfloat16), dma((2,)), dma((2,))] + [dma((4,))] * 8 + [dma((5,))] * 2,
        compiler_params=pltpu.CompilerParams(collective_id=2, has_side_effects=True),
        name='exchange',
    )(a_loc, b_loc)


def pair_kernel(a_ref, b_ref, w_ref, out_ref, at_f32, at, outer):
    def transpose_a(c, _):
        for sb in range(4):
            blk = a_ref[c, sb * 128:sb * 128 + 128, :].astype(jnp.float32).T
            at_f32[sb, pl.ds(pl.multiple_of(c * STRIDE, 8), 64), :] = blk[:64]
            at_f32[sb, pl.ds(pl.multiple_of((c + 16) * STRIDE, 8), 64), :] = blk[64:]
        return 0

    lax.fori_loop(0, 16, transpose_a, 0)

    def regroup(i, _):
        for sb in range(4):
            rows = at_f32[sb, pl.ds(i, 32, stride=STRIDE), :]
            at[pl.ds(pl.multiple_of(i * 32, 32), 32), sb * 128:sb * 128 + 128] = rows.astype(jnp.bfloat16)
        return 0

    lax.fori_loop(0, 64, regroup, 0, unroll=2)

    def products(dp, _):
        rhs = jnp.concatenate([b_ref[2 * dp], b_ref[2 * dp + 1]], axis=1)
        for mc in range(4):
            prod = jnp.dot(at[mc * 512:mc * 512 + 512, :], rhs, preferred_element_type=jnp.float32).astype(jnp.bfloat16)
            for i in range(16):
                for dd in range(2):
                    row = pl.multiple_of((2 * dp + dd) * 32, 32)
                    lane = (i % 2) * 128
                    outer[mc * 8 + i // 2, pl.ds(row, 32), lane:lane + 128] = prod[i * 32:i * 32 + 32, dd * 128:dd * 128 + 128]
        return 0

    lax.fori_loop(0, 16, products, 0)
    w = w_ref[...]

    def combine(ip, _):
        res = jnp.dot(w, outer[ip], preferred_element_type=jnp.float32)
        out_ref[2 * ip] = res[:, :128].T.astype(jnp.bfloat16)
        out_ref[2 * ip + 1] = res[:, 128:].T.astype(jnp.bfloat16)
        return 0

    lax.fori_loop(0, 32, combine, 0, unroll=2)


def pair_partial(a_full, b_full, w2):
    return pl.pallas_call(
        pair_kernel,
        out_shape=jax.ShapeDtypeStruct((64, 128, 128), jnp.bfloat16),
        scratch_shapes=[pltpu.VMEM((4, 32 * STRIDE, 128), jnp.float32), pltpu.VMEM((2048, 512), jnp.bfloat16), pltpu.VMEM((32, 1024, 256), jnp.bfloat16)],
        cost_estimate=pl.CostEstimate(flops=12_000_000_000, bytes_accessed=8_000_000, transcendentals=0),
        name='pair_partial',
    )(a_full.reshape(16, 512, 128), b_full.reshape(32, 512, 128), w2)


AXES = ((2, 1, 0), (1, 0, 2), (0, 2, 1))
SPLIT = (((0, 6), (6, 5)), ((11, 6), (17, 5)), ((22, 5), (27, 5)))


def gather_kernel(t_ref, g_ref, send_sem, recv_sem, own_sem):
    seq = lax.axis_index('seq')
    me = (seq // 16, lax.rem(seq // 4, 4), lax.rem(seq, 4))
    strides = (16, 4, 1)

    def peer(axis, step):
        pos = lax.rem(me[axis] + step + 4, 4)
        return {'seq': seq + (pos - me[axis]) * strides[axis]}

    barrier = pltpu.get_barrier_semaphore()
    for axis in range(3):
        for step in (1, -1):
            pl.semaphore_signal(barrier, inc=1, device_id=peer(axis, step), device_id_type=pl.DeviceIdType.MESH)
    pl.semaphore_wait(barrier, 6)

    def block(part, phase, shift, u0, n):
        idx = [pl.ds(me[a], 1) for a in range(3)]
        for done in range(phase):
            idx[AXES[part][done]] = pl.ds(0, 4)
        axis = AXES[part][phase]
        idx[axis] = pl.ds(lax.rem(me[axis] + shift + 4, 4), 1)
        return g_ref.at[idx[0], idx[1], idx[2], pl.ds(u0, n)]

    def message(c, part, phase, kind):
        u0, n = SPLIT[part][c]
        lo = (n + 1) // 2 if (part + c) % 2 == 0 else n // 2
        if kind == 2:
            n = lo
        elif kind == 3:
            u0, n = u0 + lo, n - lo
        return u0, n

    def copy(c, part, phase, kind, shift):
        u0, n = message(c, part, phase, kind)
        ref = block(part, phase, shift, u0, n)
        src = ref
        if phase == 0 and shift == 0:
            src = t_ref.at[:, :, :, pl.ds(u0, n)]
        return pltpu.make_async_remote_copy(
            src_ref=src, dst_ref=ref, send_sem=send_sem.at[c, part, phase, kind],
            recv_sem=recv_sem.at[c, part, phase, kind],
            device_id=peer(AXES[part][phase], 1 if kind % 2 == 0 else -1),
            device_id_type=pl.DeviceIdType.MESH)

    sent_shift = (0, 0, -1, 1)
    got_shift = (-1, 1, -2, 2)
    own = pltpu.make_async_copy(t_ref, g_ref.at[pl.ds(me[0], 1), pl.ds(me[1], 1), pl.ds(me[2], 1)], own_sem)
    order = [(c, p) for c in range(2) for p in range(3)]
    for c, p in order:
        copy(c, p, 0, 0, 0).start()
        copy(c, p, 0, 1, 0).start()
    own.start()
    own.wait()
    for phase in range(3):
        for c, p in order:
            for kind in (0, 1):
                copy(c, p, phase, kind, got_shift[kind]).wait_recv()
                copy(c, p, phase, kind + 2, sent_shift[kind + 2]).start()
        for c, p in order:
            for kind in (2, 3):
                copy(c, p, phase, kind, got_shift[kind]).wait_recv()
            if phase < 2:
                copy(c, p, phase + 1, 0, 0).start()
                copy(c, p, phase + 1, 1, 0).start()
    for phase in range(3):
        for c, p in order:
            for kind in range(4):
                copy(c, p, phase, kind, sent_shift[kind]).wait_send()


def gather(tile):
    return pl.pallas_call(
        gather_kernel,
        in_specs=[pl.BlockSpec(memory_space=pltpu.VMEM)],
        out_specs=pl.BlockSpec(memory_space=pl.ANY),
        out_shape=jax.ShapeDtypeStruct((4, 4, 4, 32, 64, 128), jnp.bfloat16),
        scratch_shapes=[pltpu.SemaphoreType.DMA((2, 3, 3, 4)), pltpu.SemaphoreType.DMA((2, 3, 3, 4)), pltpu.SemaphoreType.DMA],
        compiler_params=pltpu.CompilerParams(collective_id=1, has_side_effects=True),
        name='gather_tiles',
    )(tile.reshape(1, 1, 1, 32, 64, 128))


ROWS = 8


def update_kernel(z_ref, g_ref, inv_ref, b_ref, out_ref):
    blk = (pl.program_id(0) * 4 + pl.program_id(1)) * (16 // ROWS) + pl.program_id(2)
    shift = lax.rem(blk * ROWS, 128)
    inv = pltpu.roll(inv_ref[...], lax.rem(128 - shift, 128), 1)
    bias = b_ref[...]
    for r in range(ROWS):
        col = inv[:, r:r + 1]
        for h in range(2):
            for y in range(4):
                j0 = y * 128 + h * 64
                seg = g_ref[0, y, 0, 2 * r + h].astype(jnp.float32)
                out_ref[r, j0:j0 + 64, :] = z_ref[r, j0:j0 + 64, :] + (seg + bias) * col[j0:j0 + 64]


def update(pair_rows, gathered, inv_t, bias):
    nb = 16 // ROWS
    row_map = lambda zi, xi, ri: ((zi * 4 + xi) * nb + ri, 0, 0)
    return pl.pallas_call(
        update_kernel,
        grid=(4, 4, nb),
        in_specs=[
            pl.BlockSpec((ROWS, 512, 128), row_map),
            pl.BlockSpec((1, 4, 1, 2 * ROWS, 64, 128), lambda zi, xi, ri: (zi, 0, xi, ri, 0, 0)),
            pl.BlockSpec((512, 128), lambda zi, xi, ri: (0, zi // 2)),
            pl.BlockSpec((1, 128), lambda zi, xi, ri: (0, 0)),
        ],
        out_specs=pl.BlockSpec((ROWS, 512, 128), row_map),
        out_shape=jax.ShapeDtypeStruct(pair_rows.shape, jnp.float32),
        cost_estimate=pl.CostEstimate(flops=30_000_000_000, bytes_accessed=160_000_000, transcendentals=0),
        name='update',
    )(pair_rows, gathered, inv_t, bias)


def solution(mesh):
    rep = P()
    in_specs = (P(('data', 'seq'), 'dap', None), P('data', None), P(('data', 'dap'), None, None)) + (rep,) * 8
    out_specs = (P(('data', 'dap'), None, None), P(('data', 'seq', 'dap'), None, None))
    rng = range(4)
    xgroups = [[z * 16 + y * 4 + x for x in rng] for z in rng for y in rng]

    def local_fn(msa, mask, pair_rows, ln_gamma, ln_beta, w_left, b_left, w_right, b_right, w_out, b_out):
        seq_idx = lax.axis_index('seq')
        dap_idx = lax.axis_index('dap')
        msa_out = lax.all_to_all(msa, 'dap', 0, 1, tiled=True)
        mask_seq = lax.dynamic_slice(mask, (seq_idx * 32, dap_idx * 256), (32, 256)).astype(jnp.float32)
        col = lambda v: v.astype(jnp.float32).reshape(-1, 1)
        w_cat = jnp.concatenate([w_left, w_right], axis=1).T
        bias_cat = jnp.concatenate([col(b_left), col(b_right)], axis=0)
        a_loc, b_loc = project(jnp.swapaxes(msa, 1, 2), mask_seq, col(ln_gamma), col(ln_beta), w_cat, bias_cat)
        a_full, b_full = exchange(a_loc, b_loc)
        w2 = w_out.reshape(32, 32, 128).transpose(2, 1, 0).reshape(128, 1024)
        partial = pair_partial(a_full, b_full, w2)
        parts = lax.all_to_all(partial.reshape(4, 16, 128, 128), 'seq', 0, 0, axis_index_groups=xgroups, tiled=True)
        total = jnp.sum(parts.astype(jnp.float32), axis=0).astype(jnp.bfloat16)

        mask_bf16 = mask.astype(jnp.bfloat16)
        mask_rows = lax.dynamic_slice_in_dim(mask_bf16, dap_idx * 256, 256, axis=1)
        count_t = jnp.einsum('sj,si->ji', mask_bf16, mask_rows, preferred_element_type=jnp.float32)
        inv_t = 1.0 / (1e-3 + count_t)
        bias = b_out.astype(jnp.float32).reshape(1, 128)

        out = update(pair_rows, gather(total), inv_t, bias)
        return out, msa_out

    return jax.shard_map(local_fn, mesh=mesh, in_specs=in_specs, out_specs=out_specs, check_vma=False)
```

```python
import functools

import jax
import jax.numpy as jnp
from jax import lax
from jax.experimental import pallas as pl
from jax.experimental.pallas import tpu as pltpu
from jax.sharding import PartitionSpec as P


STRIDE = 72


def project_kernel(m_ref, mask_ref, gamma_ref, beta_ref, w_ref, bias_ref, a_ref, b_ref, scr):
    gamma, beta, bias = gamma_ref[...], beta_ref[...], bias_ref[...]
    w = w_ref[...]
    for s in range(32):
        x = m_ref[s].astype(jnp.float32)
        cen = x - jnp.mean(x, axis=0, keepdims=True)
        var = jnp.mean(cen * cen, axis=0, keepdims=True)
        normed = (cen * lax.rsqrt(var + 1e-5) * gamma + beta).astype(jnp.bfloat16)
        out = (jnp.dot(w, normed, preferred_element_type=jnp.float32) + bias) * mask_ref[s:s + 1, :]
        for t in range(2):
            scr[t, s * STRIDE:s * STRIDE + 64, :] = out[:, t * 128:t * 128 + 128]
    low = lax.broadcasted_iota(jnp.int32, (32, 128), 1) < 64
    for t in range(2):
        for c in range(16):
            lo = scr[t, pl.ds(c, 32, stride=STRIDE), :]
            hi = scr[t, pl.ds(16 + c, 32, stride=STRIDE), :]
            a_ref[2 * t, c] = jnp.where(low, lo, pltpu.roll(hi, 64, 1)).astype(jnp.bfloat16)
            a_ref[2 * t + 1, c] = jnp.where(low, pltpu.roll(lo, 64, 1), hi).astype(jnp.bfloat16)
        for d in range(32):
            b_ref[d // 16, t, d % 16] = scr[t, pl.ds(32 + d, 32, stride=STRIDE), :].astype(jnp.bfloat16)


def project(msa_t, mask_f32, gamma, beta, w_cat, bias_cat):
    return pl.pallas_call(
        project_kernel,
        out_shape=(jax.ShapeDtypeStruct((4, 16, 32, 128), jnp.bfloat16), jax.ShapeDtypeStruct((2, 2, 16, 32, 128), jnp.bfloat16)),
        scratch_shapes=[pltpu.VMEM((2, 32 * STRIDE, 128), jnp.float32)],
        name='project',
    )(msa_t, mask_f32, gamma, beta, w_cat, bias_cat)


MESH = pl.DeviceIdType.MESH


def exchange_kernel(a_in, b_in, a_out, b_out, b_mid, dap_sem, loc_sem, aa_send, aa_recv, bb_send, bb_recv, ag_send, ag_recv, bg_send, bg_recv, sib_send, sib_recv):
    seq = lax.axis_index('seq')
    core = lax.axis_index('dap')
    z, y = seq // 16, lax.rem(seq // 4, 4)

    def zpos(step):
        return lax.rem(z + step + 4, 4)

    def ypos(step):
        return lax.rem(y + step + 4, 4)

    def zpeer(step):
        return {'seq': seq + (zpos(step) - z) * 16}

    def ypeer(step):
        return {'seq': seq + (ypos(step) - y) * 4}

    sibling = {'dap': 1 - core}
    barrier = pltpu.get_barrier_semaphore()
    for peer in [zpeer(i) for i in (1, 2, 3)] + [ypeer(i) for i in (1, 2, 3)] + [sibling]:
        pl.semaphore_signal(barrier, inc=1, device_id=peer, device_id_type=MESH)
    pl.semaphore_wait(barrier, 7)

    def remote(src, dst, ssem, rsem, peer):
        return pltpu.make_async_remote_copy(src_ref=src, dst_ref=dst, send_sem=ssem, recv_sem=rsem, device_id=peer, device_id_type=MESH)

    to_sib = remote(b_in.at[1 - core], b_mid.at[pl.ds(2 * core, 2)], dap_sem.at[0], dap_sem.at[1], sibling)
    to_sib.start()
    mine_b = pltpu.make_async_copy(b_in.at[core], b_mid.at[pl.ds(2 * core, 2)], loc_sem.at[0])
    mine_b.start()
    mine_a = pltpu.make_async_copy(a_in.at[z], a_out.at[:, y, z], loc_sem.at[1])
    mine_a.start()

    def a_scatter(shift):
        return remote(a_in.at[zpos(shift)], a_out.at[:, y, z], aa_send.at[shift], aa_recv.at[shift], zpeer(shift))

    def a_scattered(shift):
        ref = a_out.at[:, y, zpos(-shift)]
        return remote(ref, ref, aa_send.at[shift], aa_recv.at[shift], zpeer(shift))

    def b_scatter(shift):
        return remote(b_mid.at[ypos(shift)], b_out.at[core, :, y, z], bb_send.at[shift], bb_recv.at[shift], ypeer(shift))

    def b_scattered(shift):
        ref = b_out.at[core, :, ypos(-shift), z]
        return remote(ref, ref, bb_send.at[shift], bb_recv.at[shift], ypeer(shift))

    for shift in (1, 3, 2):
        a_scatter(shift).start()
    got = b_mid.at[pl.ds(2 * (1 - core), 2)]
    remote(got, got, dap_sem.at[0], dap_sem.at[1], sibling).wait_recv()
    mine_b.wait()
    for shift in (1, 3, 2):
        b_scatter(shift).start()
    b_out[core, :, y, z] = b_mid[y]

    half = ((0, 16), (0, 16), (0, 8), (8, 8))
    shifts = (0, 0, -1, 1)
    landed = (-1, 1, -2, 2)

    def a_gather(kind, shift):
        c0, n = half[kind]
        ref = a_out.at[pl.ds(c0, n), ypos(shift)]
        return remote(ref, ref, ag_send.at[kind], ag_recv.at[kind], ypeer(1 if kind % 2 == 0 else -1))

    def b_gather(kind, shift):
        c0, n = half[kind]
        ref = b_out.at[core, pl.ds(c0, n), :, zpos(shift)]
        return remote(ref, ref, bg_send.at[kind], bg_recv.at[kind], zpeer(1 if kind % 2 == 0 else -1))

    def share(slot, which, shift, kind):
        c0, n = half[kind]
        ref = b_out.at[which, pl.ds(c0, n), :, zpos(shift)]
        return remote(ref, ref, sib_send.at[slot], sib_recv.at[slot], sibling)

    shared = ((0, 0), (-1, 0), (1, 0), (-2, 2), (2, 3))
    for shift in (1, 3, 2):
        a_scattered(shift).wait_recv()
    mine_a.wait()
    a_gather(0, 0).start()
    a_gather(1, 0).start()
    for shift in (1, 3, 2):
        b_scattered(shift).wait_recv()
    b_gather(0, 0).start()
    b_gather(1, 0).start()
    share(0, core, *shared[0]).start()
    for kind in (0, 1):
        a_gather(kind, landed[kind]).wait_recv()
        a_gather(kind + 2, shifts[kind + 2]).start()
        b_gather(kind, landed[kind]).wait_recv()
        b_gather(kind + 2, shifts[kind + 2]).start()
        share(kind + 1, core, *shared[kind + 1]).start()
    for kind in (2, 3):
        b_gather(kind, landed[kind]).wait_recv()
        share(kind + 1, core, *shared[kind + 1]).start()
    for kind in (2, 3):
        a_gather(kind, landed[kind]).wait_recv()
    for slot in range(5):
        share(slot, 1 - core, *shared[slot]).wait_recv()
    to_sib.wait_send()
    for shift in (1, 3, 2):
        a_scatter(shift).wait_send()
        b_scatter(shift).wait_send()
    for kind in range(4):
        a_gather(kind, shifts[kind]).wait_send()
        b_gather(kind, shifts[kind]).wait_send()
    for slot in range(5):
        share(slot, core, *shared[slot]).wait_send()


def exchange(a_loc, b_loc):
    dma = pltpu.SemaphoreType.DMA
    return pl.pallas_call(
        exchange_kernel,
        in_specs=[pl.BlockSpec(memory_space=pl.ANY)] * 2,
        out_specs=(pl.BlockSpec(memory_space=pltpu.VMEM),) * 2,
        out_shape=(jax.ShapeDtypeStruct((16, 4, 4, 32, 128), jnp.bfloat16), jax.ShapeDtypeStruct((2, 16, 4, 4, 32, 128), jnp.bfloat16)),
        scratch_shapes=[pltpu.VMEM((4, 16, 32, 128), jnp.bfloat16), dma((2,)), dma((2,))] + [dma((4,))] * 8 + [dma((5,))] * 2,
        compiler_params=pltpu.CompilerParams(collective_id=2, has_side_effects=True),
        name='exchange',
    )(a_loc, b_loc)


def pair_kernel(a_ref, b_ref, w_ref, out_ref, at_f32, at, outer):
    def transpose_a(c, _):
        for sb in range(4):
            blk = a_ref[c, sb * 128:sb * 128 + 128, :].astype(jnp.float32).T
            at_f32[sb, pl.ds(pl.multiple_of(c * STRIDE, 8), 64), :] = blk[:64]
            at_f32[sb, pl.ds(pl.multiple_of((c + 16) * STRIDE, 8), 64), :] = blk[64:]
        return 0

    lax.fori_loop(0, 16, transpose_a, 0)

    def regroup(i, _):
        for sb in range(4):
            rows = at_f32[sb, pl.ds(i, 32, stride=STRIDE), :]
            at[pl.ds(pl.multiple_of(i * 32, 32), 32), sb * 128:sb * 128 + 128] = rows.astype(jnp.bfloat16)
        return 0

    lax.fori_loop(0, 64, regroup, 0, unroll=2)

    def products(dp, _):
        rhs = jnp.concatenate([b_ref[2 * dp], b_ref[2 * dp + 1]], axis=1)
        for mc in range(4):
            prod = jnp.dot(at[mc * 512:mc * 512 + 512, :], rhs, preferred_element_type=jnp.float32).astype(jnp.bfloat16)
            for i in range(16):
                for dd in range(2):
                    row = pl.multiple_of((2 * dp + dd) * 32, 32)
                    lane = (i % 2) * 128
                    outer[mc * 8 + i // 2, pl.ds(row, 32), lane:lane + 128] = prod[i * 32:i * 32 + 32, dd * 128:dd * 128 + 128]
        return 0

    lax.fori_loop(0, 16, products, 0)
    w = w_ref[...]

    def combine(ip, _):
        res = jnp.dot(w, outer[ip], preferred_element_type=jnp.float32)
        out_ref[2 * ip] = res[:, :128].T.astype(jnp.bfloat16)
        out_ref[2 * ip + 1] = res[:, 128:].T.astype(jnp.bfloat16)
        return 0

    lax.fori_loop(0, 32, combine, 0, unroll=2)


def pair_partial(a_full, b_full, w2):
    return pl.pallas_call(
        pair_kernel,
        out_shape=jax.ShapeDtypeStruct((64, 128, 128), jnp.bfloat16),
        scratch_shapes=[pltpu.VMEM((4, 32 * STRIDE, 128), jnp.float32), pltpu.VMEM((2048, 512), jnp.bfloat16), pltpu.VMEM((32, 1024, 256), jnp.bfloat16)],
        cost_estimate=pl.CostEstimate(flops=12_000_000_000, bytes_accessed=8_000_000, transcendentals=0),
        name='pair_partial',
    )(a_full.reshape(16, 512, 128), b_full.reshape(32, 512, 128), w2)


AXES = ((2, 1, 0), (1, 0, 2), (0, 2, 1))
OTHER = ((1, 2), (0, 1), (0, 2))
ROW0 = (0, 5, 10)
HALF = ((0, 3), (3, 2))
COLS = ((0, 48), (48, 40), (88, 40))
COL_LOW = (24, 24, 16)
STRIDES = (16, 4, 1)


def coords():
    seq = lax.axis_index('seq')
    return seq // 16, lax.rem(seq // 4, 4), lax.rem(seq, 4)


def gather_kernel(t_ref, *refs):
    own = (refs[0:2], refs[2:4], refs[4:6])
    near = (refs[6:8], refs[8:10], refs[10:12])
    last_row, send_sem, recv_sem, near_send, near_recv, row_send, row_recv, own_sem = refs[12:]
    seq = lax.axis_index('seq')
    me = coords()

    def at(axis, step):
        return lax.rem(me[axis] + step + 4, 4)

    def peer(axis, step):
        return {'seq': seq + (at(axis, step) - me[axis]) * STRIDES[axis]}

    barrier = pltpu.get_barrier_semaphore()
    for axis in range(3):
        for step in (1, -1):
            pl.semaphore_signal(barrier, inc=1, device_id=peer(axis, step), device_id_type=MESH)
    pl.semaphore_wait(barrier, 6)

    def index(part, phase, shift, axes):
        idx = []
        for axis in axes:
            if axis in AXES[part][:phase]:
                idx.append(pl.ds(0, 4))
            elif axis == AXES[part][phase]:
                idx.append(pl.ds(at(axis, shift), 1))
            else:
                idx.append(pl.ds(me[axis], 1))
        return tuple(idx)

    def piece(total, low, kind):
        return ((0, total), (0, total), (0, low), (low, total - low))[kind]

    def copy(c, part, phase, kind, shift):
        to = peer(AXES[part][phase], 1 if kind % 2 == 0 else -1)
        if c == 2:
            lo, n = piece(COLS[part][1], COL_LOW[part], kind)
            ref = last_row.at[index(part, phase, shift, (0, 1, 2)) + (pl.ds(COLS[part][0] + lo, n),)]
            src = ref
            if phase == 0 and shift == 0:
                src = t_ref.at[:, :, pl.ds(15, 1), pl.ds(COLS[part][0] + lo, n)]
            sems = (row_send.at[part, phase, kind], row_recv.at[part, phase, kind])
        else:
            base, rows = HALF[c]
            lo, n = piece(rows, 2 - part % 2 if c == 0 else 1, kind)
            ref = own[part][c].at[index(part, phase, shift, OTHER[part]) + (pl.ds(lo, n),)]
            src = ref
            if phase == 0 and shift == 0:
                src = t_ref.at[:, :, pl.ds(ROW0[part] + base + lo, n)]
            sems = (send_sem.at[c, part, phase, kind], recv_sem.at[c, part, phase, kind])
        return pltpu.make_async_remote_copy(src_ref=src, dst_ref=ref, send_sem=sems[0], recv_sem=sems[1], device_id=to, device_id_type=MESH)

    def last_copy(c, part):
        to = peer(AXES[part][2], 1 if c == 0 else -1)
        return pltpu.make_async_remote_copy(src_ref=own[part][c], dst_ref=near[part][c], send_sem=near_send.at[c, part], recv_sem=near_recv.at[c, part], device_id=to, device_id_type=MESH)

    sent = (0, 0, -1, 1)
    got = (-1, 1, -2, 2)
    order = [(c, p) for c in range(3) for p in range(3)]
    for c, p in order:
        copy(c, p, 0, 0, 0).start()
        copy(c, p, 0, 1, 0).start()
    local = []
    for p in range(3):
        for c in range(2):
            dst = own[p][c].at[tuple(pl.ds(me[axis], 1) for axis in OTHER[p])]
            local.append(pltpu.make_async_copy(t_ref.at[:, :, pl.ds(ROW0[p] + HALF[c][0], HALF[c][1])], dst, own_sem.at[len(local)]))
    local.append(pltpu.make_async_copy(t_ref.at[:, :, pl.ds(15, 1)], last_row.at[tuple(pl.ds(me[axis], 1) for axis in range(3))], own_sem.at[6]))
    for item in local:
        item.start()
    for item in local:
        item.wait()
    for phase in range(3):
        active = [(c, p) for c, p in order if phase < 2 or c == 2]
        for c, p in active:
            for kind in (0, 1):
                copy(c, p, phase, kind, got[kind]).wait_recv()
                copy(c, p, phase, kind + 2, sent[kind + 2]).start()
        for c, p in active:
            for kind in (2, 3):
                copy(c, p, phase, kind, got[kind]).wait_recv()
            if phase == 0 or (phase == 1 and c == 2):
                copy(c, p, phase + 1, 0, 0).start()
                copy(c, p, phase + 1, 1, 0).start()
            elif phase == 1:
                last_copy(c, p).start()
    for c in range(2):
        for p in range(3):
            last_copy(c, p).wait_recv()
    for c, p in order:
        for phase in range(3 if c == 2 else 2):
            for kind in range(4):
                copy(c, p, phase, kind, sent[kind]).wait_send()
        if c < 2:
            last_copy(c, p).wait_send()


def gather(tile):
    halves = [jax.ShapeDtypeStruct((4, 4, HALF[c][1], 128, 128), jnp.bfloat16) for _ in range(6) for c in range(2)]
    dma = pltpu.SemaphoreType.DMA
    res = pl.pallas_call(
        gather_kernel,
        in_specs=[pl.BlockSpec(memory_space=pltpu.VMEM)],
        out_specs=[pl.BlockSpec(memory_space=pl.ANY)] * 13,
        out_shape=halves + [jax.ShapeDtypeStruct((4, 4, 4, 128, 128), jnp.bfloat16)],
        scratch_shapes=[dma((2, 3, 2, 4)), dma((2, 3, 2, 4)), dma((2, 3)), dma((2, 3)), dma((3, 3, 4)), dma((3, 3, 4)), dma((7,))],
        compiler_params=pltpu.CompilerParams(collective_id=1, has_side_effects=True),
        name='gather_tiles',
    )(tile.reshape(1, 1, 16, 128, 128))
    own = [res[2 * p:2 * p + 2] for p in range(3)]
    near = [res[6 + 2 * p:8 + 2 * p] for p in range(3)]
    return own, near, res[12]


SLOTS = 8
AHEAD = 5


def update_kernel(items, n_src, n_prev, z_ref, inv_ref, b_ref, *refs):
    srcs = refs[:n_src]
    out_ref, buf, gbuf, in_sem, out_sem = refs[n_src + n_prev:]
    me = coords()
    bias = b_ref[...]

    def place(item):
        part, shift, k = item[0], item[1], item[2]
        if part == 3:
            return k, None, None
        pos = lax.rem(me[AXES[part][2]] + shift + 4, 4)
        return ((pos, None, k), (k, None, pos), (k, pos, None))[part]

    def z_slices(ref, item, slot):
        part = item[0]
        zd, yd, xd = place(item)
        if part == 3:
            return [(ref.at[zd * 4 + x, 15], buf.at[slot, :, x]) for x in range(4)]
        if part == 2:
            return [(ref.at[pl.ds(zd * 4, 4), pl.ds(10, 5), yd], buf.at[slot])]
        return [(ref.at[zd * 4 + xd, ROW0[part] + r], buf.at[slot, :, r]) for r in range(5)]

    def g_slices(item, slot):
        part, _, k, ids = item
        if part == 3:
            return [(srcs[ids[0]].at[k, :, x], gbuf.at[slot, :, x]) for x in range(4)]
        pairs = []
        for c in range(2):
            ref = srcs[ids[c]]
            src = ref.at[:, k] if part == 0 else ref.at[k]
            pairs.append((src, gbuf.at[slot, :, pl.ds(HALF[c][0], HALF[c][1])]))
        return pairs

    def start_in(i):
        slot = i % SLOTS
        for src, dst in z_slices(z_ref, items[i], slot):
            pltpu.make_async_copy(src, dst, in_sem.at[slot, 0]).start()
        for src, dst in g_slices(items[i], slot):
            pltpu.make_async_copy(src, dst, in_sem.at[slot, 1]).start()

    def rows_of(item):
        return 4 if item[0] == 3 else 5

    def wait_in(i):
        slot = i % SLOTS
        n = rows_of(items[i])
        zb, gb = buf.at[slot, :, pl.ds(0, n)], gbuf.at[slot, :, pl.ds(0, n)]
        pltpu.make_async_copy(zb, zb, in_sem.at[slot, 0]).wait()
        pltpu.make_async_copy(gb, gb, in_sem.at[slot, 1]).wait()

    def start_out(i):
        slot = i % SLOTS
        for dst, src in z_slices(out_ref, items[i], slot):
            pltpu.make_async_copy(src, dst, out_sem.at[slot]).start()

    def wait_out(i):
        slot = i % SLOTS
        zb = buf.at[slot, :, pl.ds(0, rows_of(items[i]))]
        pltpu.make_async_copy(zb, zb, out_sem.at[slot]).wait()

    def compute(i):
        slot = i % SLOTS
        item = items[i]
        part = item[0]
        zd, yd, xd = place(item)

        def body(q, _):
            if part == 3:
                lane, yq, offs = zd * 64 + 15, q, (0, 16, 32, 48)
            elif part == 2:
                lane, yq, offs = zd * 64 + q * 16 + 10, yd, (0, 1, 2, 3, 4)
            else:
                lane, yq, offs = zd * 64 + xd * 16 + ROW0[part], q, (0, 1, 2, 3, 4)
            inv = inv_ref[lane // 128, pl.ds(pl.multiple_of(yq * 128, 128), 128), :]
            inv = pltpu.roll(inv, lax.rem(256 - lane, 128), 1)
            for r, off in enumerate(offs):
                seg = gbuf[slot, q, r].astype(jnp.float32)
                buf[slot, q, r] = buf[slot, q, r] + (seg + bias) * inv[:, off:off + 1]
            return 0

        lax.fori_loop(0, 4, body, 0)

    n = len(items)
    for i in range(min(AHEAD, n)):
        start_in(i)
    for i in range(n):
        j = i + AHEAD
        if j < n:
            if j >= SLOTS:
                wait_out(j - SLOTS)
            start_in(j)
        wait_in(i)
        compute(i)
        start_out(i)
    for i in range(max(0, n - SLOTS), n):
        wait_out(i)


def update(name, items, pair5, inv2, bias, srcs, prev):
    any_spec = pl.BlockSpec(memory_space=pl.ANY)
    vmem_spec = pl.BlockSpec(memory_space=pltpu.VMEM)
    args = [pair5, inv2, bias] + srcs + ([] if prev is None else [prev])
    blocks = sum(4 if item[0] == 3 else 5 for item in items) * 4
    return pl.pallas_call(
        functools.partial(update_kernel, items, len(srcs), len(args) - 3 - len(srcs)),
        in_specs=[any_spec, vmem_spec, vmem_spec] + [any_spec] * (len(args) - 3),
        out_specs=any_spec,
        out_shape=jax.ShapeDtypeStruct(pair5.shape, jnp.float32),
        scratch_shapes=[pltpu.VMEM((SLOTS, 4, 5, 128, 128), jnp.float32), pltpu.VMEM((SLOTS, 4, 5, 128, 128), jnp.bfloat16), pltpu.SemaphoreType.DMA((SLOTS, 2)), pltpu.SemaphoreType.DMA((SLOTS,))],
        input_output_aliases={} if prev is None else {len(args) - 1: 0},
        cost_estimate=pl.CostEstimate(flops=blocks * 40_000_000, bytes_accessed=blocks * 163840, transcendentals=0),
        name=name,
    )(*args)


def ring(axis, step):
    out = []
    for i in range(64):
        pos = i // STRIDES[axis] % 4
        out.append((i, i + ((pos + step) % 4 - pos) * STRIDES[axis]))
    return out


def gather_and_update(tile, pair_rows, inv2, bias):
    own, near, last_row = gather(tile)
    pair5 = pair_rows.reshape(16, 16, 4, 128, 128)
    minus, plus, far = [], [], []
    for p in range(3):
        axis = AXES[p][2]
        minus.append([near[p][0], lax.ppermute(own[p][1], 'seq', ring(axis, 1))])
        plus.append([lax.ppermute(own[p][0], 'seq', ring(axis, -1)), near[p][1]])
    for p in range(3):
        axis = AXES[p][2]
        far.append([lax.ppermute(near[p][0], 'seq', ring(axis, 1)), lax.ppermute(near[p][1], 'seq', ring(axis, -1))])

    def items(stages):
        return [(p, shift, k, (base + 2 * p, base + 2 * p + 1)) for base, shift in stages for p in range(3) for k in range(4)]

    flat = lambda pairs: [x for pair in pairs for x in pair]
    first = [(3, 0, k, (6,)) for k in range(4)] + items([(0, 0)])
    out = update('update_own', first, pair5, inv2, bias, flat(own) + [last_row], None)
    out = update('update_near', items([(0, -1), (6, 1)]), pair5, inv2, bias, flat(minus) + flat(plus), out)
    out = update('update_far', items([(0, 2)]), pair5, inv2, bias, flat(far), out)
    return out.reshape(pair_rows.shape)


def solution(mesh):
    rep = P()
    in_specs = (P(('data', 'seq'), 'dap', None), P('data', None), P(('data', 'dap'), None, None)) + (rep,) * 8
    out_specs = (P(('data', 'dap'), None, None), P(('data', 'seq', 'dap'), None, None))
    rng = range(4)
    xgroups = [[z * 16 + y * 4 + x for x in rng] for z in rng for y in rng]

    def local_fn(msa, mask, pair_rows, ln_gamma, ln_beta, w_left, b_left, w_right, b_right, w_out, b_out):
        seq_idx = lax.axis_index('seq')
        dap_idx = lax.axis_index('dap')
        msa_out = lax.all_to_all(msa, 'dap', 0, 1, tiled=True)
        mask_seq = lax.dynamic_slice(mask, (seq_idx * 32, dap_idx * 256), (32, 256)).astype(jnp.float32)
        col = lambda v: v.astype(jnp.float32).reshape(-1, 1)
        w_cat = jnp.concatenate([w_left, w_right], axis=1).T
        bias_cat = jnp.concatenate([col(b_left), col(b_right)], axis=0)
        a_loc, b_loc = project(jnp.swapaxes(msa, 1, 2), mask_seq, col(ln_gamma), col(ln_beta), w_cat, bias_cat)
        a_full, b_full = exchange(a_loc, b_loc)
        w2 = w_out.reshape(32, 32, 128).transpose(2, 1, 0).reshape(128, 1024)
        partial = pair_partial(a_full, b_full, w2)
        parts = lax.all_to_all(partial.reshape(4, 16, 128, 128), 'seq', 0, 0, axis_index_groups=xgroups, tiled=True)
        total = jnp.sum(parts.astype(jnp.float32), axis=0).astype(jnp.bfloat16)

        mask_bf16 = mask.astype(jnp.bfloat16)
        mask_rows = lax.dynamic_slice_in_dim(mask_bf16, dap_idx * 256, 256, axis=1)
        count_t = jnp.einsum('sj,sti->tji', mask_bf16, mask_rows.reshape(2048, 2, 128), preferred_element_type=jnp.float32)
        inv2 = 1.0 / (1e-3 + count_t)
        bias = b_out.astype(jnp.float32).reshape(1, 128)

        total, inv2, bias, msa_out = lax.optimization_barrier((total, inv2, bias, msa_out))
        out = gather_and_update(total, pair_rows, inv2, bias)
        return out, msa_out

    return jax.shard_map(local_fn, mesh=mesh, in_specs=in_specs, out_specs=out_specs, check_vma=False)
```

```python
import functools

import jax
import jax.numpy as jnp
from jax import lax
from jax.experimental import pallas as pl
from jax.experimental.pallas import tpu as pltpu
from jax.sharding import PartitionSpec as P


N3, N4, N5, N8, N16, N32, N64, N128, N256, N512 = 3, 4, 5, 8, 16, 32, 64, 128, 256, 512
STRIDE = 72


def project_kernel(m_ref, mask_hbm, vec_ref, w_ref, a_ref, b_ref, scr, mask_i32, sem):
    row = pl.multiple_of(lax.axis_index('seq') * N32, N32)
    lane = pl.multiple_of(lax.axis_index('dap') * N256, N256)
    load = pltpu.make_async_copy(mask_hbm.at[pl.ds(row, N32), pl.ds(lane, N256)], mask_i32, sem)
    load.start()
    vecs = vec_ref[...].T
    gamma, beta, bias = vecs[:N64, 0:1], vecs[:N64, 1:2], vecs[:N64, 2:N3]
    w = w_ref[...]
    load.wait()
    for s in range(N32):
        x = m_ref[s].astype(jnp.float32)
        cen = x - jnp.mean(x, axis=0, keepdims=True)
        var = jnp.mean(cen * cen, axis=0, keepdims=True)
        normed = (cen * lax.rsqrt(var + 1e-5) * gamma + beta).astype(jnp.bfloat16)
        out = (jnp.dot(w, normed, preferred_element_type=jnp.float32) + bias) * mask_i32[s:s + 1, :].astype(jnp.float32)
        for t in range(2):
            scr[t, s * STRIDE:s * STRIDE + N64, :] = out[:, t * N128:t * N128 + N128]
    low = lax.broadcasted_iota(jnp.int32, (N32, N128), 1) < N64
    for t in range(2):
        for c in range(N16):
            lo = scr[t, pl.ds(c, N32, stride=STRIDE), :]
            hi = scr[t, pl.ds(N16 + c, N32, stride=STRIDE), :]
            a_ref[2 * t, c] = jnp.where(low, lo, pltpu.roll(hi, N64, 1)).astype(jnp.bfloat16)
            a_ref[2 * t + 1, c] = jnp.where(low, pltpu.roll(lo, N64, 1), hi).astype(jnp.bfloat16)
        for d in range(N32):
            b_ref[d // N16, t, d % N16] = scr[t, pl.ds(N32 + d, N32, stride=STRIDE), :].astype(jnp.bfloat16)


def project(msa_t, mask, vecs, w_cat):
    vmem_spec = pl.BlockSpec(memory_space=pltpu.VMEM)
    return pl.pallas_call(
        project_kernel,
        in_specs=[vmem_spec, pl.BlockSpec(memory_space=pl.ANY), vmem_spec, vmem_spec],
        out_shape=(jax.ShapeDtypeStruct((N4, N16, N32, N128), jnp.bfloat16), jax.ShapeDtypeStruct((2, 2, N16, N32, N128), jnp.bfloat16)),
        scratch_shapes=[pltpu.VMEM((2, N32 * STRIDE, N128), jnp.float32), pltpu.VMEM((N32, N256), jnp.int32), pltpu.SemaphoreType.DMA],
        name='project',
    )(msa_t, mask, vecs, w_cat)


MESH = pl.DeviceIdType.MESH


def exchange_kernel(a_in, b_in, m_in, a_out, b_out, m_out, b_mid, m_mid, m_sem, dap_sem, loc_sem, aa_send, aa_recv, bb_send, bb_recv, ag_send, ag_recv, bg_send, bg_recv, sib_send, sib_recv):
    seq = lax.axis_index('seq')
    core = lax.axis_index('dap')
    z, y = seq // N16, lax.rem(seq // N4, N4)

    def zpos(step):
        return lax.rem(z + step + N4, N4)

    def ypos(step):
        return lax.rem(y + step + N4, N4)

    def zpeer(step):
        return {'seq': seq + (zpos(step) - z) * N16}

    def ypeer(step):
        return {'seq': seq + (ypos(step) - y) * N4}

    sibling = {'dap': 1 - core}
    barrier = pltpu.get_barrier_semaphore()
    for peer in [zpeer(i) for i in (1, 2, N3)] + [ypeer(i) for i in (1, 2, N3)] + [sibling]:
        pl.semaphore_signal(barrier, inc=1, device_id=peer, device_id_type=MESH)
    pl.semaphore_wait(barrier, 7)

    def remote(src, dst, ssem, rsem, peer):
        return pltpu.make_async_remote_copy(src_ref=src, dst_ref=dst, send_sem=ssem, recv_sem=rsem, device_id=peer, device_id_type=MESH)

    to_sib = remote(b_in.at[1 - core], b_mid.at[pl.ds(2 * core, 2)], dap_sem.at[0], dap_sem.at[1], sibling)
    to_sib.start()
    mine_b = pltpu.make_async_copy(b_in.at[core], b_mid.at[pl.ds(2 * core, 2)], loc_sem.at[0])
    mine_b.start()
    mine_a = pltpu.make_async_copy(a_in.at[z], a_out.at[:, y, z], loc_sem.at[1])
    mine_a.start()

    def a_scatter(shift):
        return remote(a_in.at[zpos(shift)], a_out.at[:, y, z], aa_send.at[shift], aa_recv.at[shift], zpeer(shift))

    def a_scattered(shift):
        ref = a_out.at[:, y, zpos(-shift)]
        return remote(ref, ref, aa_send.at[shift], aa_recv.at[shift], zpeer(shift))

    def b_scatter(shift):
        return remote(b_mid.at[ypos(shift)], b_out.at[core, :, y, z], bb_send.at[shift], bb_recv.at[shift], ypeer(shift))

    def b_scattered(shift):
        ref = b_out.at[core, :, ypos(-shift), z]
        return remote(ref, ref, bb_send.at[shift], bb_recv.at[shift], ypeer(shift))

    for shift in (1, N3, 2):
        a_scatter(shift).start()
    half_cols = m_out.at[:, :, pl.ds(pl.multiple_of(core * N256, N256), N256)]
    m_far = remote(m_in.at[pl.ds(N16 * (1 - core), N16)], half_cols, m_sem.at[0], m_sem.at[1], sibling)
    m_far.start()
    m_load = pltpu.make_async_copy(m_in.at[pl.ds(N16 * core, N16)], m_mid, m_sem.at[2])
    m_load.start()
    m_load.wait()
    m_store = pltpu.make_async_copy(m_mid, half_cols, m_sem.at[N3])
    m_store.start()
    got = b_mid.at[pl.ds(2 * (1 - core), 2)]
    remote(got, got, dap_sem.at[0], dap_sem.at[1], sibling).wait_recv()
    mine_b.wait()
    for shift in (1, N3, 2):
        b_scatter(shift).start()
    b_out[core, :, y, z] = b_mid[y]

    half = ((0, N16), (0, N16), (0, N8), (N8, N8))
    shifts = (0, 0, -1, 1)
    landed = (-1, 1, -2, 2)

    def a_gather(kind, shift):
        c0, n = half[kind]
        ref = a_out.at[pl.ds(c0, n), ypos(shift)]
        return remote(ref, ref, ag_send.at[kind], ag_recv.at[kind], ypeer(1 if kind % 2 == 0 else -1))

    def b_gather(kind, shift):
        c0, n = half[kind]
        ref = b_out.at[core, pl.ds(c0, n), :, zpos(shift)]
        return remote(ref, ref, bg_send.at[kind], bg_recv.at[kind], zpeer(1 if kind % 2 == 0 else -1))

    def share(slot, which, shift, kind):
        c0, n = half[kind]
        ref = b_out.at[which, pl.ds(c0, n), :, zpos(shift)]
        return remote(ref, ref, sib_send.at[slot], sib_recv.at[slot], sibling)

    shared = ((0, 0), (-1, 0), (1, 0), (-2, 2), (2, N3))
    for shift in (1, N3, 2):
        a_scattered(shift).wait_recv()
    mine_a.wait()
    a_gather(0, 0).start()
    a_gather(1, 0).start()
    for shift in (1, N3, 2):
        b_scattered(shift).wait_recv()
    b_gather(0, 0).start()
    b_gather(1, 0).start()
    share(0, core, *shared[0]).start()
    for kind in (0, 1):
        a_gather(kind, landed[kind]).wait_recv()
        a_gather(kind + 2, shifts[kind + 2]).start()
        b_gather(kind, landed[kind]).wait_recv()
        b_gather(kind + 2, shifts[kind + 2]).start()
        share(kind + 1, core, *shared[kind + 1]).start()
    for kind in (2, N3):
        b_gather(kind, landed[kind]).wait_recv()
        share(kind + 1, core, *shared[kind + 1]).start()
    for kind in (2, N3):
        a_gather(kind, landed[kind]).wait_recv()
    for slot in range(N5):
        share(slot, 1 - core, *shared[slot]).wait_recv()
    to_sib.wait_send()
    m_store.wait()
    other_cols = m_out.at[:, :, pl.ds(pl.multiple_of((1 - core) * N256, N256), N256)]
    remote(other_cols, other_cols, m_sem.at[0], m_sem.at[1], sibling).wait_recv()
    m_far.wait_send()
    for shift in (1, N3, 2):
        a_scatter(shift).wait_send()
        b_scatter(shift).wait_send()
    for kind in range(N4):
        a_gather(kind, shifts[kind]).wait_send()
        b_gather(kind, shifts[kind]).wait_send()
    for slot in range(N5):
        share(slot, core, *shared[slot]).wait_send()


def exchange(a_loc, b_loc, msa_t):
    dma = pltpu.SemaphoreType.DMA
    return pl.pallas_call(
        exchange_kernel,
        in_specs=[pl.BlockSpec(memory_space=pl.ANY)] * N3,
        out_specs=(pl.BlockSpec(memory_space=pltpu.VMEM),) * 2 + (pl.BlockSpec(memory_space=pl.ANY),),
        out_shape=(jax.ShapeDtypeStruct((N16, N4, N4, N32, N128), jnp.bfloat16), jax.ShapeDtypeStruct((2, N16, N4, N4, N32, N128), jnp.bfloat16), jax.ShapeDtypeStruct((N16, N64, N512), jnp.bfloat16)),
        scratch_shapes=[pltpu.VMEM((N4, N16, N32, N128), jnp.bfloat16), pltpu.VMEM((N16, N64, N256), jnp.bfloat16), dma((N4,)), dma((2,)), dma((2,))] + [dma((N4,))] * N8 + [dma((N5,))] * 2,
        compiler_params=pltpu.CompilerParams(collective_id=2, has_side_effects=True),
        name='exchange',
    )(a_loc, b_loc, msa_t)


def pair_kernel(a_ref, b_ref, w_ref, out_ref, at_f32, at, outer):
    def transpose_a(c, _):
        for sb in range(N4):
            blk = a_ref[c, sb * N128:sb * N128 + N128, :].astype(jnp.float32).T
            at_f32[sb, pl.ds(pl.multiple_of(c * STRIDE, N8), N64), :] = blk[:N64]
            at_f32[sb, pl.ds(pl.multiple_of((c + N16) * STRIDE, N8), N64), :] = blk[N64:]
        return 0

    lax.fori_loop(0, N16, transpose_a, 0)

    def regroup(i, _):
        for sb in range(N4):
            rows = at_f32[sb, pl.ds(i, N32, stride=STRIDE), :]
            at[pl.ds(pl.multiple_of(i * N32, N32), N32), sb * N128:sb * N128 + N128] = rows.astype(jnp.bfloat16)
        return 0

    lax.fori_loop(0, N64, regroup, 0, unroll=2)

    def products(dp, _):
        rhs = jnp.concatenate([b_ref[2 * dp], b_ref[2 * dp + 1]], axis=1)
        for mc in range(N4):
            prod = jnp.dot(at[mc * N512:mc * N512 + N512, :], rhs, preferred_element_type=jnp.float32).astype(jnp.bfloat16)
            for i in range(N16):
                for dd in range(2):
                    row = pl.multiple_of((2 * dp + dd) * N32, N32)
                    lane = (i % 2) * N128
                    outer[mc * N8 + i // 2, pl.ds(row, N32), lane:lane + N128] = prod[i * N32:i * N32 + N32, dd * N128:dd * N128 + N128]
        return 0

    lax.fori_loop(0, N16, products, 0)
    w = w_ref[...]

    def combine(ip, _):
        res = jnp.dot(w, outer[ip], preferred_element_type=jnp.float32)
        out_ref[2 * ip] = res[:, :N128].T.astype(jnp.bfloat16)
        out_ref[2 * ip + 1] = res[:, N128:].T.astype(jnp.bfloat16)
        return 0

    lax.fori_loop(0, N32, combine, 0, unroll=2)


def pair_partial(a_full, b_full, w2):
    return pl.pallas_call(
        pair_kernel,
        out_shape=jax.ShapeDtypeStruct((N64, N128, N128), jnp.bfloat16),
        scratch_shapes=[pltpu.VMEM((N4, N32 * STRIDE, N128), jnp.float32), pltpu.VMEM((2048, N512), jnp.bfloat16), pltpu.VMEM((N32, 1024, N256), jnp.bfloat16)],
        cost_estimate=pl.CostEstimate(flops=12_000_000_000, bytes_accessed=8_000_000, transcendentals=0),
        name='pair_partial',
    )(a_full.reshape(N16, N512, N128), b_full.reshape(N32, N512, N128), w2)


AXES = ((2, 1, 0), (1, 0, 2), (0, 2, 1))
OTHER = ((1, 2), (0, 1), (0, 2))
ROW0 = (0, N5, 10)
HALF = ((0, N3), (N3, 2))
COLS = ((0, 48), (48, 40), (88, 40))
COL_LOW = (24, 24, N16)
STRIDES = (N16, N4, 1)


def coords():
    seq = lax.axis_index('seq')
    return seq // N16, lax.rem(seq // N4, N4), lax.rem(seq, N4)


def gather_kernel(t_ref, *refs):
    own = (refs[0:2], refs[2:N4], refs[N4:6])
    near = (refs[6:N8], refs[N8:10], refs[10:12])
    last_row, send_sem, recv_sem, near_send, near_recv, row_send, row_recv, own_sem = refs[12:]
    seq = lax.axis_index('seq')
    me = coords()

    def at(axis, step):
        return lax.rem(me[axis] + step + N4, N4)

    def peer(axis, step):
        return {'seq': seq + (at(axis, step) - me[axis]) * STRIDES[axis]}

    barrier = pltpu.get_barrier_semaphore()
    for axis in range(N3):
        for step in (1, -1):
            pl.semaphore_signal(barrier, inc=1, device_id=peer(axis, step), device_id_type=MESH)
    pl.semaphore_wait(barrier, 6)

    def index(part, phase, shift, axes):
        idx = []
        for axis in axes:
            if axis in AXES[part][:phase]:
                idx.append(pl.ds(0, N4))
            elif axis == AXES[part][phase]:
                idx.append(pl.ds(at(axis, shift), 1))
            else:
                idx.append(pl.ds(me[axis], 1))
        return tuple(idx)

    def piece(total, low, kind):
        return ((0, total), (0, total), (0, low), (low, total - low))[kind]

    def copy(c, part, phase, kind, shift):
        to = peer(AXES[part][phase], 1 if kind % 2 == 0 else -1)
        if c == 2:
            lo, n = piece(COLS[part][1], COL_LOW[part], kind)
            ref = last_row.at[index(part, phase, shift, (0, 1, 2)) + (pl.ds(COLS[part][0] + lo, n),)]
            src = ref
            if phase == 0 and shift == 0:
                src = t_ref.at[:, :, pl.ds(15, 1), pl.ds(COLS[part][0] + lo, n)]
            sems = (row_send.at[part, phase, kind], row_recv.at[part, phase, kind])
        else:
            base, rows = HALF[c]
            lo, n = piece(rows, 2 - part % 2 if c == 0 else 1, kind)
            ref = own[part][c].at[index(part, phase, shift, OTHER[part]) + (pl.ds(lo, n),)]
            src = ref
            if phase == 0 and shift == 0:
                src = t_ref.at[:, :, pl.ds(ROW0[part] + base + lo, n)]
            sems = (send_sem.at[c, part, phase, kind], recv_sem.at[c, part, phase, kind])
        return pltpu.make_async_remote_copy(src_ref=src, dst_ref=ref, send_sem=sems[0], recv_sem=sems[1], device_id=to, device_id_type=MESH)

    sent = (0, 0, -1, 1)
    got = (-1, 1, -2, 2)
    quarter = (0, -1, 1, -2)

    def last_copy(c, part, k):
        to = peer(AXES[part][2], 1 if c == 0 else -1)
        idx = index(part, 1, quarter[k], OTHER[part])
        return pltpu.make_async_remote_copy(src_ref=own[part][c].at[idx], dst_ref=near[part][c].at[idx], send_sem=near_send.at[c, part, k], recv_sem=near_recv.at[c, part, k], device_id=to, device_id_type=MESH)

    mains = [(c, p) for c in range(2) for p in range(N3)]
    order = [(c, p) for c in range(N3) for p in range(N3)]
    for c, p in order:
        copy(c, p, 0, 0, 0).start()
        copy(c, p, 0, 1, 0).start()
    local = []
    for p in range(N3):
        for c in range(2):
            dst = own[p][c].at[tuple(pl.ds(me[axis], 1) for axis in OTHER[p])]
            local.append(pltpu.make_async_copy(t_ref.at[:, :, pl.ds(ROW0[p] + HALF[c][0], HALF[c][1])], dst, own_sem.at[len(local)]))
    local.append(pltpu.make_async_copy(t_ref.at[:, :, pl.ds(15, 1)], last_row.at[tuple(pl.ds(me[axis], 1) for axis in range(N3))], own_sem.at[6]))
    for item in local:
        item.start()
    for item in local:
        item.wait()
    for phase in range(N3):
        active = [(c, p) for c, p in order if phase < 2 or c == 2]
        for c, p in active:
            for kind in (0, 1):
                copy(c, p, phase, kind, got[kind]).wait_recv()
                copy(c, p, phase, kind + 2, sent[kind + 2]).start()
                if phase == 1 and c < 2:
                    last_copy(c, p, kind + 1).start()
        for c, p in active:
            for kind in (2, N3):
                copy(c, p, phase, kind, got[kind]).wait_recv()
            if phase == 0 or (phase == 1 and c == 2):
                copy(c, p, phase + 1, 0, 0).start()
                copy(c, p, phase + 1, 1, 0).start()
            elif phase == 1:
                last_copy(c, p, N3).start()
        if phase == 0:
            for c, p in mains:
                last_copy(c, p, 0).start()
    for c, p in mains:
        for k in range(N4):
            last_copy(c, p, k).wait_recv()
    for c, p in order:
        for phase in range(N3 if c == 2 else 2):
            for kind in range(N4):
                copy(c, p, phase, kind, sent[kind]).wait_send()
        if c < 2:
            for k in range(N4):
                last_copy(c, p, k).wait_send()


def gather(tile):
    halves = [jax.ShapeDtypeStruct((N4, N4, HALF[c][1], N128, N128), jnp.bfloat16) for _ in range(6) for c in range(2)]
    dma = pltpu.SemaphoreType.DMA
    res = pl.pallas_call(
        gather_kernel,
        in_specs=[pl.BlockSpec(memory_space=pltpu.VMEM)],
        out_specs=[pl.BlockSpec(memory_space=pl.ANY)] * 13,
        out_shape=halves + [jax.ShapeDtypeStruct((N4, N4, N4, N128, N128), jnp.bfloat16)],
        scratch_shapes=[dma((2, N3, 2, N4)), dma((2, N3, 2, N4)), dma((2, N3, N4)), dma((2, N3, N4)), dma((N3, N3, N4)), dma((N3, N3, N4)), dma((7,))],
        compiler_params=pltpu.CompilerParams(collective_id=1, has_side_effects=True),
        name='gather_tiles',
    )(tile.reshape(1, 1, N16, N128, N128))
    own = [res[2 * p:2 * p + 2] for p in range(N3)]
    near = [res[6 + 2 * p:N8 + 2 * p] for p in range(N3)]
    return own, near, res[12]


SLOTS = N8
AHEAD = 6


def update_kernel(items, n_src, n_prev, z_ref, inv_ref, b_ref, *refs):
    srcs = refs[:n_src]
    out_ref, buf, gbuf, in_sem, out_sem = refs[n_src + n_prev:]
    me = coords()
    bias = b_ref[...]

    def place(item):
        part, shift, k = item[0], item[1], item[2]
        if part == N3:
            return k, None, None
        pos = lax.rem(me[AXES[part][2]] + shift + N4, N4)
        return ((pos, None, k), (k, None, pos), (k, pos, None))[part]

    def rows_of(item):
        if item[0] == N3:
            return 0, N4
        used = [c for c in range(2) if item[N3][c] is not None]
        return HALF[used[0]][0], sum(HALF[c][1] for c in used)

    def z_slices(ref, item, slot):
        part = item[0]
        zd, yd, xd = place(item)
        if part == N3:
            return [(ref.at[zd * N4 + x, 15], buf.at[slot, :, x]) for x in range(N4)]
        lo, n = rows_of(item)
        lo = ROW0[part] + lo
        if part == 2:
            return [(ref.at[pl.ds(zd * N4, N4), pl.ds(lo, n), yd], buf.at[slot, :, pl.ds(0, n)])]
        return [(ref.at[zd * N4 + xd, lo + r], buf.at[slot, :, r]) for r in range(n)]

    def g_slices(item, slot):
        part, _, k, ids = item
        if part == N3:
            return [(srcs[ids[0]].at[k, :, x], gbuf.at[slot, :, x]) for x in range(N4)]
        pairs = []
        lo = rows_of(item)[0]
        for c in range(2):
            if ids[c] is not None:
                ref = srcs[ids[c]]
                src = ref.at[:, k] if part == 0 else ref.at[k]
                pairs.append((src, gbuf.at[slot, :, pl.ds(HALF[c][0] - lo, HALF[c][1])]))
        return pairs

    def start_in(i):
        slot = i % SLOTS
        for src, dst in z_slices(z_ref, items[i], slot):
            pltpu.make_async_copy(src, dst, in_sem.at[slot, 0]).start()
        for src, dst in g_slices(items[i], slot):
            pltpu.make_async_copy(src, dst, in_sem.at[slot, 1]).start()

    def wait_in(i):
        slot = i % SLOTS
        n = rows_of(items[i])[1]
        zb, gb = buf.at[slot, :, pl.ds(0, n)], gbuf.at[slot, :, pl.ds(0, n)]
        pltpu.make_async_copy(zb, zb, in_sem.at[slot, 0]).wait()
        pltpu.make_async_copy(gb, gb, in_sem.at[slot, 1]).wait()

    def start_out(i):
        slot = i % SLOTS
        for dst, src in z_slices(out_ref, items[i], slot):
            pltpu.make_async_copy(src, dst, out_sem.at[slot]).start()

    def wait_out(i):
        slot = i % SLOTS
        zb = buf.at[slot, :, pl.ds(0, rows_of(items[i])[1])]
        pltpu.make_async_copy(zb, zb, out_sem.at[slot]).wait()

    def compute(i):
        slot = i % SLOTS
        item = items[i]
        part = item[0]
        zd, yd, xd = place(item)

        lo, n = rows_of(item)
        offs = tuple(x * N16 for x in range(N4)) if part == N3 else tuple(range(n))

        def body(q, _):
            lane, yq = zd * N64, q
            if part == N3:
                lane = lane + 15
            elif part == 2:
                lane, yq = lane + q * N16 + ROW0[part] + lo, yd
            else:
                lane = lane + xd * N16 + ROW0[part] + lo
            inv = inv_ref[lane // N128, pl.ds(pl.multiple_of(yq * N128, N128), N128), :]
            inv = pltpu.roll(inv, lax.rem(N256 - lane, N128), 1)
            for r, off in enumerate(offs):
                seg = gbuf[slot, q, r].astype(jnp.float32)
                buf[slot, q, r] = buf[slot, q, r] + (seg + bias) * inv[:, off:off + 1]
            return 0

        lax.fori_loop(0, N4, body, 0)

    n = len(items)
    for i in range(min(AHEAD, n)):
        start_in(i)
    for i in range(n):
        j = i + AHEAD
        if j < n:
            if j >= SLOTS:
                wait_out(j - SLOTS)
            start_in(j)
        wait_in(i)
        compute(i)
        start_out(i)
    for i in range(max(0, n - SLOTS), n):
        wait_out(i)


def update(name, items, pair5, inv2, bias, srcs, prev):
    any_spec = pl.BlockSpec(memory_space=pl.ANY)
    vmem_spec = pl.BlockSpec(memory_space=pltpu.VMEM)
    args = [pair5, inv2, bias] + srcs + ([] if prev is None else [prev])
    blocks = len(items) * N16
    return pl.pallas_call(
        functools.partial(update_kernel, items, len(srcs), len(args) - N3 - len(srcs)),
        in_specs=[any_spec, vmem_spec, vmem_spec] + [any_spec] * (len(args) - N3),
        out_specs=any_spec,
        out_shape=jax.ShapeDtypeStruct(pair5.shape, jnp.float32),
        scratch_shapes=[pltpu.VMEM((SLOTS, N4, N5, N128, N128), jnp.float32), pltpu.VMEM((SLOTS, N4, N5, N128, N128), jnp.bfloat16), pltpu.SemaphoreType.DMA((SLOTS, 2)), pltpu.SemaphoreType.DMA((SLOTS,))],
        input_output_aliases={} if prev is None else {len(args) - 1: 0},
        cost_estimate=pl.CostEstimate(flops=blocks * 40_000_000, bytes_accessed=blocks * 163840, transcendentals=0),
        name=name,
    )(*args)


def ring(axis, step):
    out = []
    for i in range(N64):
        pos = i // STRIDES[axis] % N4
        out.append((i, i + ((pos + step) % N4 - pos) * STRIDES[axis]))
    return out


def gather_and_update(tile, pair_rows, inv2, bias):
    own, near, last_row = gather(tile)
    pair5 = pair_rows.reshape(N16, N16, N4, N128, N128)
    minus, plus, far = [], [], []
    for p in range(N3):
        axis = AXES[p][2]
        minus.append(lax.ppermute(own[p][1], 'seq', ring(axis, 1)))
        plus.append(lax.ppermute(own[p][0], 'seq', ring(axis, -1)))
    for p in range(N3):
        axis = AXES[p][2]
        far.append([lax.ppermute(near[p][0], 'seq', ring(axis, 1)), lax.ppermute(near[p][1], 'seq', ring(axis, -1))])

    def items(shift, low, high):
        ids = lambda p: tuple(None if base is None else base + p for base in (low, high))
        return [(p, shift, k, ids(p)) for p in range(N3) for k in range(N4)]

    col = lambda pairs, c: [pair[c] for pair in pairs]
    srcs = [last_row] + col(own, 0) + col(own, 1) + col(near, 0) + col(near, 1)
    work = [(N3, 0, k, (0,)) for k in range(N4)] + items(0, 1, N4) + items(-1, 7, None) + items(1, None, 10)
    out = update('update_own', work, pair5, inv2, bias, srcs, None)
    work = items(-1, None, 0) + items(2, None, N3)
    out = update('update_near', work, pair5, inv2, bias, minus + col(far, 1), out)
    work = items(1, 0, None) + items(2, N3, None)
    out = update('update_far', work, pair5, inv2, bias, plus + col(far, 0), out)
    return out.reshape(pair_rows.shape)


def solution(mesh):
    rep = P()
    in_specs = (P(('data', 'seq'), 'dap', None), P('data', None), P(('data', 'dap'), None, None)) + (rep,) * N8
    out_specs = (P(('data', 'dap'), None, None), P(('data', 'seq', 'dap'), None, None))
    rng = range(N4)
    xgroups = [[z * N16 + y * N4 + x for x in rng] for z in rng for y in rng]

    def local_fn(msa, mask, pair_rows, ln_gamma, ln_beta, w_left, b_left, w_right, b_right, w_out, b_out):
        dap_idx = lax.axis_index('dap')
        msa_t = jnp.swapaxes(msa, 1, 2)
        rows = jnp.stack([ln_gamma, ln_beta, jnp.concatenate([b_left, b_right])]).astype(jnp.float32)
        vecs = jnp.pad(rows, ((0, N5), (0, N64)))
        w_cat = jnp.concatenate([w_left, w_right], axis=1).T
        a_loc, b_loc = project(msa_t, mask, vecs, w_cat)
        a_full, b_full, m_full = exchange(a_loc, b_loc, msa_t)
        msa_out = jnp.swapaxes(m_full, 1, 2)
        w2 = w_out.reshape(N32, N32, N128).transpose(2, 1, 0).reshape(N128, 1024)
        partial = pair_partial(a_full, b_full, w2)
        parts = lax.all_to_all(partial.reshape(N4, N16, N128, N128), 'seq', 0, 0, axis_index_groups=xgroups, tiled=True)
        total = jnp.sum(parts.astype(jnp.float32), axis=0).astype(jnp.bfloat16)

        mask_bf16 = mask.astype(jnp.bfloat16)
        mask_rows = lax.dynamic_slice_in_dim(mask_bf16, dap_idx * N256, N256, axis=1)
        count_t = jnp.einsum('sj,sti->tji', mask_bf16, mask_rows.reshape(2048, 2, N128), preferred_element_type=jnp.float32)
        inv2 = 1.0 / (1e-3 + count_t)
        bias = b_out.astype(jnp.float32).reshape(1, N128)

        total, inv2, bias = lax.optimization_barrier((total, inv2, bias))
        out = gather_and_update(total, pair_rows, inv2, bias)
        return out, msa_out

    return jax.shard_map(local_fn, mesh=mesh, in_specs=in_specs, out_specs=out_specs, check_vma=False)
```

```python
import functools

import jax
import jax.numpy as jnp
from jax import lax
from jax.experimental import pallas as pl
from jax.experimental.pallas import tpu as pltpu
from jax.sharding import PartitionSpec as P


N3, N4, N5, N8, N16, N32, N64, N128, N256, N512 = 3, 4, 5, 8, 16, 32, 64, 128, 256, 512
STRIDE = 72


def project_kernel(m_ref, mask_hbm, vec_ref, w_ref, a_ref, b_ref, scr, mask_i32, sem):
    row = pl.multiple_of(lax.axis_index('seq') * N32, N32)
    lane = pl.multiple_of(lax.axis_index('dap') * N256, N256)
    load = pltpu.make_async_copy(mask_hbm.at[pl.ds(row, N32), pl.ds(lane, N256)], mask_i32, sem)
    load.start()
    vecs = vec_ref[...].T
    gamma, beta, bias = vecs[:N64, 0:1], vecs[:N64, 1:2], vecs[:N64, 2:N3]
    w = w_ref[...]
    load.wait()
    for s in range(N32):
        x = m_ref[s].astype(jnp.float32)
        cen = x - jnp.mean(x, axis=0, keepdims=True)
        var = jnp.mean(cen * cen, axis=0, keepdims=True)
        normed = (cen * lax.rsqrt(var + 1e-5) * gamma + beta).astype(jnp.bfloat16)
        out = (jnp.dot(w, normed, preferred_element_type=jnp.float32) + bias) * mask_i32[s:s + 1, :].astype(jnp.float32)
        for t in range(2):
            scr[t, s * STRIDE:s * STRIDE + N64, :] = out[:, t * N128:t * N128 + N128]
    low = lax.broadcasted_iota(jnp.int32, (N32, N128), 1) < N64
    for t in range(2):
        for c in range(N16):
            lo = scr[t, pl.ds(c, N32, stride=STRIDE), :]
            hi = scr[t, pl.ds(N16 + c, N32, stride=STRIDE), :]
            a_ref[2 * t, c] = jnp.where(low, lo, pltpu.roll(hi, N64, 1)).astype(jnp.bfloat16)
            a_ref[2 * t + 1, c] = jnp.where(low, pltpu.roll(lo, N64, 1), hi).astype(jnp.bfloat16)
        for d in range(N32):
            b_ref[d // N16, t, d % N16] = scr[t, pl.ds(N32 + d, N32, stride=STRIDE), :].astype(jnp.bfloat16)


def project(msa_t, mask, vecs, w_cat):
    vmem_spec = pl.BlockSpec(memory_space=pltpu.VMEM)
    return pl.pallas_call(
        project_kernel,
        in_specs=[vmem_spec, pl.BlockSpec(memory_space=pl.ANY), vmem_spec, vmem_spec],
        out_shape=(jax.ShapeDtypeStruct((N4, N16, N32, N128), jnp.bfloat16), jax.ShapeDtypeStruct((2, 2, N16, N32, N128), jnp.bfloat16)),
        scratch_shapes=[pltpu.VMEM((2, N32 * STRIDE, N128), jnp.float32), pltpu.VMEM((N32, N256), jnp.int32), pltpu.SemaphoreType.DMA],
        name='project',
    )(msa_t, mask, vecs, w_cat)


MESH = pl.DeviceIdType.MESH


def exchange_kernel(a_in, b_in, m_in, a_out, b_out, m_out, b_mid, m_mid, m_sem, dap_sem, loc_sem, aa_send, aa_recv, bb_send, bb_recv, ag_send, ag_recv, bg_send, bg_recv, sib_send, sib_recv):
    seq = lax.axis_index('seq')
    core = lax.axis_index('dap')
    z, y = seq // N16, lax.rem(seq // N4, N4)

    def zpos(step):
        return lax.rem(z + step + N4, N4)

    def ypos(step):
        return lax.rem(y + step + N4, N4)

    def zpeer(step):
        return {'seq': seq + (zpos(step) - z) * N16}

    def ypeer(step):
        return {'seq': seq + (ypos(step) - y) * N4}

    sibling = {'dap': 1 - core}
    barrier = pltpu.get_barrier_semaphore()
    for peer in [zpeer(i) for i in (1, 2, N3)] + [ypeer(i) for i in (1, 2, N3)] + [sibling]:
        pl.semaphore_signal(barrier, inc=1, device_id=peer, device_id_type=MESH)
    pl.semaphore_wait(barrier, 7)

    def remote(src, dst, ssem, rsem, peer):
        return pltpu.make_async_remote_copy(src_ref=src, dst_ref=dst, send_sem=ssem, recv_sem=rsem, device_id=peer, device_id_type=MESH)

    to_sib = remote(b_in.at[1 - core], b_mid.at[pl.ds(2 * core, 2)], dap_sem.at[0], dap_sem.at[1], sibling)
    to_sib.start()
    mine_b = pltpu.make_async_copy(b_in.at[core], b_mid.at[pl.ds(2 * core, 2)], loc_sem.at[0])
    mine_b.start()
    mine_a = pltpu.make_async_copy(a_in.at[z], a_out.at[:, y, z], loc_sem.at[1])
    mine_a.start()

    def a_scatter(shift):
        return remote(a_in.at[zpos(shift)], a_out.at[:, y, z], aa_send.at[shift], aa_recv.at[shift], zpeer(shift))

    def a_scattered(shift):
        ref = a_out.at[:, y, zpos(-shift)]
        return remote(ref, ref, aa_send.at[shift], aa_recv.at[shift], zpeer(shift))

    def b_scatter(shift):
        return remote(b_mid.at[ypos(shift)], b_out.at[core, :, y, z], bb_send.at[shift], bb_recv.at[shift], ypeer(shift))

    def b_scattered(shift):
        ref = b_out.at[core, :, ypos(-shift), z]
        return remote(ref, ref, bb_send.at[shift], bb_recv.at[shift], ypeer(shift))

    for shift in (1, N3, 2):
        a_scatter(shift).start()
    half_cols = m_out.at[:, :, pl.ds(pl.multiple_of(core * N256, N256), N256)]
    m_far = remote(m_in.at[pl.ds(N16 * (1 - core), N16)], half_cols, m_sem.at[0], m_sem.at[1], sibling)
    m_far.start()
    m_load = pltpu.make_async_copy(m_in.at[pl.ds(N16 * core, N16)], m_mid, m_sem.at[2])
    m_load.start()
    m_load.wait()
    m_store = pltpu.make_async_copy(m_mid, half_cols, m_sem.at[N3])
    m_store.start()
    got = b_mid.at[pl.ds(2 * (1 - core), 2)]
    remote(got, got, dap_sem.at[0], dap_sem.at[1], sibling).wait_recv()
    mine_b.wait()
    for shift in (1, N3, 2):
        b_scatter(shift).start()
    b_out[core, :, y, z] = b_mid[y]

    half = ((0, N16), (0, N16), (0, N8), (N8, N8))
    shifts = (0, 0, -1, 1)
    landed = (-1, 1, -2, 2)

    def a_gather(kind, shift):
        c0, n = half[kind]
        ref = a_out.at[pl.ds(c0, n), ypos(shift)]
        return remote(ref, ref, ag_send.at[kind], ag_recv.at[kind], ypeer(1 if kind % 2 == 0 else -1))

    def b_gather(kind, shift):
        c0, n = half[kind]
        ref = b_out.at[core, pl.ds(c0, n), :, zpos(shift)]
        return remote(ref, ref, bg_send.at[kind], bg_recv.at[kind], zpeer(1 if kind % 2 == 0 else -1))

    def share(slot, which, shift, kind):
        c0, n = half[kind]
        ref = b_out.at[which, pl.ds(c0, n), :, zpos(shift)]
        return remote(ref, ref, sib_send.at[slot], sib_recv.at[slot], sibling)

    shared = ((0, 0), (-1, 0), (1, 0), (-2, 2), (2, N3))
    for shift in (1, N3, 2):
        a_scattered(shift).wait_recv()
    mine_a.wait()
    a_gather(0, 0).start()
    a_gather(1, 0).start()
    for shift in (1, N3, 2):
        b_scattered(shift).wait_recv()
    b_gather(0, 0).start()
    b_gather(1, 0).start()
    share(0, core, *shared[0]).start()
    for kind in (0, 1):
        a_gather(kind, landed[kind]).wait_recv()
        a_gather(kind + 2, shifts[kind + 2]).start()
        b_gather(kind, landed[kind]).wait_recv()
        b_gather(kind + 2, shifts[kind + 2]).start()
        share(kind + 1, core, *shared[kind + 1]).start()
    for kind in (2, N3):
        b_gather(kind, landed[kind]).wait_recv()
        share(kind + 1, core, *shared[kind + 1]).start()
    for kind in (2, N3):
        a_gather(kind, landed[kind]).wait_recv()
    for slot in range(N5):
        share(slot, 1 - core, *shared[slot]).wait_recv()
    to_sib.wait_send()
    m_store.wait()
    other_cols = m_out.at[:, :, pl.ds(pl.multiple_of((1 - core) * N256, N256), N256)]
    remote(other_cols, other_cols, m_sem.at[0], m_sem.at[1], sibling).wait_recv()
    m_far.wait_send()
    for shift in (1, N3, 2):
        a_scatter(shift).wait_send()
        b_scatter(shift).wait_send()
    for kind in range(N4):
        a_gather(kind, shifts[kind]).wait_send()
        b_gather(kind, shifts[kind]).wait_send()
    for slot in range(N5):
        share(slot, core, *shared[slot]).wait_send()


def exchange(a_loc, b_loc, msa_t):
    dma = pltpu.SemaphoreType.DMA
    return pl.pallas_call(
        exchange_kernel,
        in_specs=[pl.BlockSpec(memory_space=pl.ANY)] * N3,
        out_specs=(pl.BlockSpec(memory_space=pltpu.VMEM),) * 2 + (pl.BlockSpec(memory_space=pl.ANY),),
        out_shape=(jax.ShapeDtypeStruct((N16, N4, N4, N32, N128), jnp.bfloat16), jax.ShapeDtypeStruct((2, N16, N4, N4, N32, N128), jnp.bfloat16), jax.ShapeDtypeStruct((N16, N64, N512), jnp.bfloat16)),
        scratch_shapes=[pltpu.VMEM((N4, N16, N32, N128), jnp.bfloat16), pltpu.VMEM((N16, N64, N256), jnp.bfloat16), dma((N4,)), dma((2,)), dma((2,))] + [dma((N4,))] * N8 + [dma((N5,))] * 2,
        compiler_params=pltpu.CompilerParams(collective_id=2, has_side_effects=True),
        name='exchange',
    )(a_loc, b_loc, msa_t)


def pair_kernel(a_ref, b_ref, w_ref, out_ref, at_f32, at, outer):
    def transpose_a(c, _):
        for sb in range(N4):
            blk = a_ref[c, sb * N128:sb * N128 + N128, :].astype(jnp.float32).T
            at_f32[sb, pl.ds(pl.multiple_of(c * STRIDE, N8), N64), :] = blk[:N64]
            at_f32[sb, pl.ds(pl.multiple_of((c + N16) * STRIDE, N8), N64), :] = blk[N64:]
        return 0

    lax.fori_loop(0, N16, transpose_a, 0)

    def regroup(i, _):
        for sb in range(N4):
            rows = at_f32[sb, pl.ds(i, N32, stride=STRIDE), :]
            at[pl.ds(pl.multiple_of(i * N32, N32), N32), sb * N128:sb * N128 + N128] = rows.astype(jnp.bfloat16)
        return 0

    lax.fori_loop(0, N64, regroup, 0, unroll=2)

    def products(dp, _):
        rhs = jnp.concatenate([b_ref[2 * dp], b_ref[2 * dp + 1]], axis=1)
        for mc in range(N4):
            prod = jnp.dot(at[mc * N512:mc * N512 + N512, :], rhs, preferred_element_type=jnp.float32).astype(jnp.bfloat16)
            for i in range(N16):
                for dd in range(2):
                    row = pl.multiple_of((2 * dp + dd) * N32, N32)
                    lane = (i % 2) * N128
                    outer[mc * N8 + i // 2, pl.ds(row, N32), lane:lane + N128] = prod[i * N32:i * N32 + N32, dd * N128:dd * N128 + N128]
        return 0

    lax.fori_loop(0, N16, products, 0)
    w = w_ref[...]

    def combine(ip, _):
        res = jnp.dot(w, outer[ip], preferred_element_type=jnp.float32)
        out_ref[2 * ip] = res[:, :N128].T.astype(jnp.bfloat16)
        out_ref[2 * ip + 1] = res[:, N128:].T.astype(jnp.bfloat16)
        return 0

    lax.fori_loop(0, N32, combine, 0, unroll=2)


def pair_partial(a_full, b_full, w2):
    return pl.pallas_call(
        pair_kernel,
        out_shape=jax.ShapeDtypeStruct((N64, N128, N128), jnp.bfloat16),
        scratch_shapes=[pltpu.VMEM((N4, N32 * STRIDE, N128), jnp.float32), pltpu.VMEM((2048, N512), jnp.bfloat16), pltpu.VMEM((N32, 1024, N256), jnp.bfloat16)],
        cost_estimate=pl.CostEstimate(flops=12_000_000_000, bytes_accessed=8_000_000, transcendentals=0),
        name='pair_partial',
    )(a_full.reshape(N16, N512, N128), b_full.reshape(N32, N512, N128), w2)


AXES = ((2, 1, 0), (1, 0, 2), (0, 2, 1))
OTHER = ((1, 2), (0, 1), (0, 2))
ROW0 = (0, N5, 10)
HALF = ((0, N3), (N3, 2))
COLS = ((0, 48), (48, 40), (88, 40))
COL_LOW = (24, 24, N16)
STRIDES = (N16, N4, 1)


def coords():
    seq = lax.axis_index('seq')
    return seq // N16, lax.rem(seq // N4, N4), lax.rem(seq, N4)


def gather_kernel(t_ref, *refs):
    own, near = refs[0:N3], refs[N3:6]
    last_row, send_sem, recv_sem, near_send, near_recv, row_send, row_recv, own_sem = refs[6:]
    seq = lax.axis_index('seq')
    onward = 1 - 2 * lax.axis_index('dap')
    me = coords()

    def at(axis, step):
        return lax.rem(me[axis] + step + N4, N4)

    def peer(axis, step):
        return {'seq': seq + (at(axis, step) - me[axis]) * STRIDES[axis]}

    barrier = pltpu.get_barrier_semaphore()
    for axis in range(N3):
        for step in (1, -1):
            pl.semaphore_signal(barrier, inc=1, device_id=peer(axis, step), device_id_type=MESH)
    pl.semaphore_wait(barrier, 6)

    def index(part, phase, shift, axes):
        idx = []
        for axis in axes:
            if axis in AXES[part][:phase]:
                idx.append(pl.ds(0, N4))
            elif axis == AXES[part][phase]:
                idx.append(pl.ds(at(axis, shift), 1))
            else:
                idx.append(pl.ds(me[axis], 1))
        return tuple(idx)

    def piece(total, low, kind):
        return ((0, total), (0, total), (0, low), (low, total - low))[kind]

    def copy(c, part, phase, kind, shift):
        to = peer(AXES[part][phase], 1 if kind % 2 == 0 else -1)
        if c == 2:
            lo, n = piece(COLS[part][1], COL_LOW[part], kind)
            ref = last_row.at[index(part, phase, shift, (0, 1, 2)) + (pl.ds(COLS[part][0] + lo, n),)]
            src = ref
            if phase == 0 and shift == 0:
                src = t_ref.at[:, :, pl.ds(15, 1), pl.ds(COLS[part][0] + lo, n)]
            sems = (row_send.at[part, phase, kind], row_recv.at[part, phase, kind])
        else:
            base, rows = HALF[c]
            lo, n = piece(rows, 2 - part % 2 if c == 0 else 1, kind)
            ref = own[part].at[index(part, phase, shift, OTHER[part]) + (pl.ds(base + lo, n),)]
            src = ref
            if phase == 0 and shift == 0:
                src = t_ref.at[:, :, pl.ds(ROW0[part] + base + lo, n)]
            sems = (send_sem.at[c, part, phase, kind], recv_sem.at[c, part, phase, kind])
        return pltpu.make_async_remote_copy(src_ref=src, dst_ref=ref, send_sem=sems[0], recv_sem=sems[1], device_id=to, device_id_type=MESH)

    sent = (0, 0, -1, 1)
    got = (-1, 1, -2, 2)

    def last_copy(c, part):
        to = peer(AXES[part][2], onward)
        idx = (slice(None), slice(None), pl.ds(*HALF[c]))
        return pltpu.make_async_remote_copy(src_ref=own[part].at[idx], dst_ref=near[part].at[idx], send_sem=near_send.at[c, part], recv_sem=near_recv.at[c, part], device_id=to, device_id_type=MESH)

    mains = [(c, p) for c in range(2) for p in range(N3)]
    order = [(c, p) for c in range(N3) for p in range(N3)]
    for c, p in order:
        copy(c, p, 0, 0, 0).start()
        copy(c, p, 0, 1, 0).start()
    local = []
    for p in range(N3):
        dst = own[p].at[tuple(pl.ds(me[axis], 1) for axis in OTHER[p])]
        local.append(pltpu.make_async_copy(t_ref.at[:, :, pl.ds(ROW0[p], N5)], dst, own_sem.at[p]))
    local.append(pltpu.make_async_copy(t_ref.at[:, :, pl.ds(15, 1)], last_row.at[tuple(pl.ds(me[axis], 1) for axis in range(N3))], own_sem.at[N3]))
    for item in local:
        item.start()
    for item in local:
        item.wait()
    for phase in range(N3):
        active = [(c, p) for c, p in order if phase < 2 or c == 2]
        for c, p in active:
            for kind in (0, 1):
                copy(c, p, phase, kind, got[kind]).wait_recv()
                copy(c, p, phase, kind + 2, sent[kind + 2]).start()
        for c, p in active:
            for kind in (2, N3):
                copy(c, p, phase, kind, got[kind]).wait_recv()
            if phase == 0 or (phase == 1 and c == 2):
                copy(c, p, phase + 1, 0, 0).start()
                copy(c, p, phase + 1, 1, 0).start()
            elif phase == 1:
                last_copy(c, p).start()
    for c, p in mains:
        last_copy(c, p).wait_recv()
    for c, p in order:
        for phase in range(N3 if c == 2 else 2):
            for kind in range(N4):
                copy(c, p, phase, kind, sent[kind]).wait_send()
        if c < 2:
            last_copy(c, p).wait_send()


def gather(tile):
    parts = [jax.ShapeDtypeStruct((N4, N4, N5, N128, N128), jnp.bfloat16) for _ in range(6)]
    dma = pltpu.SemaphoreType.DMA
    res = pl.pallas_call(
        gather_kernel,
        in_specs=[pl.BlockSpec(memory_space=pltpu.VMEM)],
        out_specs=[pl.BlockSpec(memory_space=pl.ANY)] * 7,
        out_shape=parts + [jax.ShapeDtypeStruct((N4, N4, N4, N128, N128), jnp.bfloat16)],
        scratch_shapes=[dma((2, N3, 2, N4)), dma((2, N3, 2, N4)), dma((2, N3)), dma((2, N3)), dma((N3, N3, N4)), dma((N3, N3, N4)), dma((N4,))],
        compiler_params=pltpu.CompilerParams(collective_id=1, has_side_effects=True),
        name='gather_tiles',
    )(tile.reshape(1, 1, N16, N128, N128))
    return res[0:N3], res[N3:6], res[6]


SLOTS = 12
AHEAD = N8


def update_kernel(items, n_src, n_prev, z_ref, inv_ref, b_ref, *refs):
    srcs = refs[:n_src]
    out_ref, buf, gbuf, in_sem, out_sem = refs[n_src + n_prev:]
    me = coords()
    bias = b_ref[...]
    onward = 1 - 2 * lax.axis_index('dap')

    def place(item):
        part, shift, k = item[0], item[1], item[2]
        if part == N3:
            return k, None, None
        pos = lax.rem(me[AXES[part][2]] + shift * onward + N4, N4)
        return ((pos, None, k), (k, None, pos), (k, pos, None))[part]

    def rows_of(item):
        return N4 if item[0] == N3 else N5

    def z_slices(ref, item, slot):
        part = item[0]
        zd, yd, xd = place(item)
        if part == N3:
            return [(ref.at[zd * N4 + x, 15], buf.at[slot, :, x]) for x in range(N4)]
        if part == 2:
            return [(ref.at[pl.ds(zd * N4, N4), pl.ds(ROW0[part], N5), yd], buf.at[slot])]
        return [(ref.at[zd * N4 + xd, ROW0[part] + r], buf.at[slot, :, r]) for r in range(N5)]

    def g_slices(item, slot):
        part, _, k, src = item
        ref = srcs[src]
        if part == N3:
            return [(ref.at[k, :, x], gbuf.at[slot, :, x]) for x in range(N4)]
        return [(ref.at[:, k] if part == 0 else ref.at[k], gbuf.at[slot])]

    def start_in(i):
        slot = i % SLOTS
        for src, dst in z_slices(z_ref, items[i], slot):
            pltpu.make_async_copy(src, dst, in_sem.at[slot, 0]).start()
        for src, dst in g_slices(items[i], slot):
            pltpu.make_async_copy(src, dst, in_sem.at[slot, 1]).start()

    def wait_in(i):
        slot = i % SLOTS
        n = rows_of(items[i])
        zb, gb = buf.at[slot, :, pl.ds(0, n)], gbuf.at[slot, :, pl.ds(0, n)]
        pltpu.make_async_copy(zb, zb, in_sem.at[slot, 0]).wait()
        pltpu.make_async_copy(gb, gb, in_sem.at[slot, 1]).wait()

    def start_out(i):
        slot = i % SLOTS
        for dst, src in z_slices(out_ref, items[i], slot):
            pltpu.make_async_copy(src, dst, out_sem.at[slot]).start()

    def wait_out(i):
        slot = i % SLOTS
        zb = buf.at[slot, :, pl.ds(0, rows_of(items[i]))]
        pltpu.make_async_copy(zb, zb, out_sem.at[slot]).wait()

    def compute(i):
        slot = i % SLOTS
        item = items[i]
        part = item[0]
        zd, yd, xd = place(item)

        offs = tuple(x * N16 for x in range(N4)) if part == N3 else tuple(range(N5))

        def body(q, _):
            lane, yq = zd * N64, q
            if part == N3:
                lane = lane + 15
            elif part == 2:
                lane, yq = lane + q * N16 + ROW0[part], yd
            else:
                lane = lane + xd * N16 + ROW0[part]
            inv = inv_ref[lane // N128, pl.ds(pl.multiple_of(yq * N128, N128), N128), :]
            inv = pltpu.roll(inv, lax.rem(N256 - lane, N128), 1)
            for r, off in enumerate(offs):
                seg = gbuf[slot, q, r].astype(jnp.float32)
                buf[slot, q, r] = buf[slot, q, r] + (seg + bias) * inv[:, off:off + 1]
            return 0

        lax.fori_loop(0, N4, body, 0)

    n = len(items)
    for i in range(min(AHEAD, n)):
        start_in(i)
    for i in range(n):
        j = i + AHEAD
        if j < n:
            if j >= SLOTS:
                wait_out(j - SLOTS)
            start_in(j)
        wait_in(i)
        compute(i)
        start_out(i)
    for i in range(max(0, n - SLOTS), n):
        wait_out(i)


def update(name, items, pair5, inv2, bias, srcs, prev):
    any_spec = pl.BlockSpec(memory_space=pl.ANY)
    vmem_spec = pl.BlockSpec(memory_space=pltpu.VMEM)
    args = [pair5, inv2, bias] + srcs + ([] if prev is None else [prev])
    blocks = len(items) * N16
    return pl.pallas_call(
        functools.partial(update_kernel, items, len(srcs), len(args) - N3 - len(srcs)),
        in_specs=[any_spec, vmem_spec, vmem_spec] + [any_spec] * (len(args) - N3),
        out_specs=any_spec,
        out_shape=jax.ShapeDtypeStruct(pair5.shape, jnp.float32),
        scratch_shapes=[pltpu.VMEM((SLOTS, N4, N5, N128, N128), jnp.float32), pltpu.VMEM((SLOTS, N4, N5, N128, N128), jnp.bfloat16), pltpu.SemaphoreType.DMA((SLOTS, 2)), pltpu.SemaphoreType.DMA((SLOTS,))],
        input_output_aliases={} if prev is None else {len(args) - 1: 0},
        cost_estimate=pl.CostEstimate(flops=blocks * 40_000_000, bytes_accessed=blocks * 163840, transcendentals=0),
        name=name,
    )(*args)


def ring(axis, step):
    out = []
    for i in range(N64):
        pos = i // STRIDES[axis] % N4
        for core in range(2):
            to = i + ((pos + step * (1 - 2 * core)) % N4 - pos) * STRIDES[axis]
            out.append((2 * i + core, 2 * to + core))
    return out


def gather_and_update(tile, pair_rows, inv2, bias):
    own, near, last_row = gather(tile)
    pair5 = pair_rows.reshape(N16, N16, N4, N128, N128)
    send = lambda x, p, step: lax.ppermute(x, ('seq', 'dap'), ring(AXES[p][2], step))
    items = lambda shift, base: [(p, shift, k, base + p) for p in range(N3) for k in range(N4)]
    ahead = [send(own[p], p, -1) for p in range(N3)]
    first = [(N3, 0, k, N3) for k in range(N4)] + items(0, 0)
    out = update('update_own', first, pair5, inv2, bias, list(own) + [last_row], None)
    near, out = lax.optimization_barrier((near, out))
    far = [send(near[p], p, 1) for p in range(N3)]
    out = update('update_behind', items(-1, 0), pair5, inv2, bias, list(near), out)
    out = update('update_ahead', items(1, 0), pair5, inv2, bias, ahead, out)
    out = update('update_far', items(2, 0), pair5, inv2, bias, far, out)
    return out.reshape(pair_rows.shape)


def solution(mesh):
    rep = P()
    in_specs = (P(('data', 'seq'), 'dap', None), P('data', None), P(('data', 'dap'), None, None)) + (rep,) * N8
    out_specs = (P(('data', 'dap'), None, None), P(('data', 'seq', 'dap'), None, None))
    rng = range(N4)
    xgroups = [[z * N16 + y * N4 + x for x in rng] for z in rng for y in rng]

    def local_fn(msa, mask, pair_rows, ln_gamma, ln_beta, w_left, b_left, w_right, b_right, w_out, b_out):
        dap_idx = lax.axis_index('dap')
        msa_t = jnp.swapaxes(msa, 1, 2)
        rows = jnp.stack([ln_gamma, ln_beta, jnp.concatenate([b_left, b_right])]).astype(jnp.float32)
        vecs = jnp.pad(rows, ((0, N5), (0, N64)))
        w_cat = jnp.concatenate([w_left, w_right], axis=1).T
        a_loc, b_loc = project(msa_t, mask, vecs, w_cat)
        a_full, b_full, m_full = exchange(a_loc, b_loc, msa_t)
        msa_out = jnp.swapaxes(m_full, 1, 2)
        w2 = w_out.reshape(N32, N32, N128).transpose(2, 1, 0).reshape(N128, 1024)
        partial = pair_partial(a_full, b_full, w2)
        parts = lax.all_to_all(partial.reshape(N4, N16, N128, N128), 'seq', 0, 0, axis_index_groups=xgroups, tiled=True)
        total = jnp.sum(parts.astype(jnp.float32), axis=0).astype(jnp.bfloat16)

        mask_bf16 = mask.astype(jnp.bfloat16)
        mask_rows = lax.dynamic_slice_in_dim(mask_bf16, dap_idx * N256, N256, axis=1)
        count_t = jnp.einsum('sj,sti->tji', mask_bf16, mask_rows.reshape(2048, 2, N128), preferred_element_type=jnp.float32)
        inv2 = 1.0 / (1e-3 + count_t)
        bias = b_out.astype(jnp.float32).reshape(1, N128)

        total, inv2, bias = lax.optimization_barrier((total, inv2, bias))
        out = gather_and_update(total, pair_rows, inv2, bias)
        return out, msa_out

    return jax.shard_map(local_fn, mesh=mesh, in_specs=in_specs, out_specs=out_specs, check_vma=False)
```

```python
import functools

import jax
import jax.numpy as jnp
from jax import lax
from jax.experimental import pallas as pl
from jax.experimental.pallas import tpu as pltpu
from jax.sharding import PartitionSpec as P


N3, N4, N5, N8, N16, N32, N64, N128, N256, N512 = 3, 4, 5, 8, 16, 32, 64, 128, 256, 512
STRIDE = 72


def project_kernel(m_ref, mask_hbm, vec_ref, wl_ref, wr_ref, a_ref, b_ref, scr, mask_i32, sem):
    row = pl.multiple_of(lax.axis_index('seq') * N32, N32)
    lane = pl.multiple_of(lax.axis_index('dap') * N256, N256)
    load = pltpu.make_async_copy(mask_hbm.at[pl.ds(row, N32), pl.ds(lane, N256)], mask_i32, sem)
    load.start()
    vecs = vec_ref[...].T
    gamma, beta, bias = vecs[:N64, 0:1], vecs[:N64, 1:2], vecs[:N64, 2:N3]
    w = jnp.concatenate([wl_ref[...], wr_ref[...]], axis=0)
    load.wait()
    for s in range(N32):
        x = m_ref[s].astype(jnp.float32)
        cen = x - jnp.mean(x, axis=0, keepdims=True)
        var = jnp.mean(cen * cen, axis=0, keepdims=True)
        normed = (cen * lax.rsqrt(var + 1e-5) * gamma + beta).astype(jnp.bfloat16)
        out = (jnp.dot(w, normed, preferred_element_type=jnp.float32) + bias) * mask_i32[s:s + 1, :].astype(jnp.float32)
        for t in range(2):
            scr[t, s * STRIDE:s * STRIDE + N64, :] = out[:, t * N128:t * N128 + N128]
    low = lax.broadcasted_iota(jnp.int32, (N32, N128), 1) < N64
    for t in range(2):
        for c in range(N16):
            lo = scr[t, pl.ds(c, N32, stride=STRIDE), :]
            hi = scr[t, pl.ds(N16 + c, N32, stride=STRIDE), :]
            a_ref[2 * t, c] = jnp.where(low, lo, pltpu.roll(hi, N64, 1)).astype(jnp.bfloat16)
            a_ref[2 * t + 1, c] = jnp.where(low, pltpu.roll(lo, N64, 1), hi).astype(jnp.bfloat16)
        for d in range(N32):
            b_ref[d // N16, t, d % N16] = scr[t, pl.ds(N32 + d, N32, stride=STRIDE), :].astype(jnp.bfloat16)


def project(msa_t, mask, vecs, w_l, w_r):
    vmem_spec = pl.BlockSpec(memory_space=pltpu.VMEM)
    return pl.pallas_call(
        project_kernel,
        in_specs=[vmem_spec, pl.BlockSpec(memory_space=pl.ANY), vmem_spec, vmem_spec, vmem_spec],
        out_shape=(jax.ShapeDtypeStruct((N4, N16, N32, N128), jnp.bfloat16), jax.ShapeDtypeStruct((2, 2, N16, N32, N128), jnp.bfloat16)),
        scratch_shapes=[pltpu.VMEM((2, N32 * STRIDE, N128), jnp.float32), pltpu.VMEM((N32, N256), jnp.int32), pltpu.SemaphoreType.DMA],
        name='project',
    )(msa_t, mask, vecs, w_l, w_r)


MESH = pl.DeviceIdType.MESH


def exchange_kernel(a_in, b_in, m_in, a_out, b_out, m_out, b_mid, m_mid, m_sem, dap_sem, loc_sem, aa_send, aa_recv, bb_send, bb_recv, ag_send, ag_recv, bg_send, bg_recv, sib_send, sib_recv):
    seq = lax.axis_index('seq')
    core = lax.axis_index('dap')
    z, y = seq // N16, lax.rem(seq // N4, N4)

    def zpos(step):
        return lax.rem(z + step + N4, N4)

    def ypos(step):
        return lax.rem(y + step + N4, N4)

    def zpeer(step):
        return {'seq': seq + (zpos(step) - z) * N16}

    def ypeer(step):
        return {'seq': seq + (ypos(step) - y) * N4}

    sibling = {'dap': 1 - core}
    barrier = pltpu.get_barrier_semaphore()
    for peer in [zpeer(i) for i in (1, 2, N3)] + [ypeer(i) for i in (1, 2, N3)] + [sibling]:
        pl.semaphore_signal(barrier, inc=1, device_id=peer, device_id_type=MESH)
    pl.semaphore_wait(barrier, 7)

    def remote(src, dst, ssem, rsem, peer):
        return pltpu.make_async_remote_copy(src_ref=src, dst_ref=dst, send_sem=ssem, recv_sem=rsem, device_id=peer, device_id_type=MESH)

    to_sib = remote(b_in.at[1 - core], b_mid.at[pl.ds(2 * core, 2)], dap_sem.at[0], dap_sem.at[1], sibling)
    to_sib.start()
    mine_b = pltpu.make_async_copy(b_in.at[core], b_mid.at[pl.ds(2 * core, 2)], loc_sem.at[0])
    mine_b.start()
    mine_a = pltpu.make_async_copy(a_in.at[z], a_out.at[:, y, z], loc_sem.at[1])
    mine_a.start()

    def a_scatter(shift):
        return remote(a_in.at[zpos(shift)], a_out.at[:, y, z], aa_send.at[shift], aa_recv.at[shift], zpeer(shift))

    def a_scattered(shift):
        ref = a_out.at[:, y, zpos(-shift)]
        return remote(ref, ref, aa_send.at[shift], aa_recv.at[shift], zpeer(shift))

    def b_scatter(shift):
        return remote(b_mid.at[ypos(shift)], b_out.at[core, :, y, z], bb_send.at[shift], bb_recv.at[shift], ypeer(shift))

    def b_scattered(shift):
        ref = b_out.at[core, :, ypos(-shift), z]
        return remote(ref, ref, bb_send.at[shift], bb_recv.at[shift], ypeer(shift))

    for shift in (1, N3, 2):
        a_scatter(shift).start()
    half_cols = m_out.at[:, :, pl.ds(pl.multiple_of(core * N256, N256), N256)]
    m_far = remote(m_in.at[pl.ds(N16 * (1 - core), N16)], half_cols, m_sem.at[0], m_sem.at[1], sibling)
    m_far.start()
    m_load = pltpu.make_async_copy(m_in.at[pl.ds(N16 * core, N16)], m_mid, m_sem.at[2])
    m_load.start()
    m_load.wait()
    m_store = pltpu.make_async_copy(m_mid, half_cols, m_sem.at[N3])
    m_store.start()
    got = b_mid.at[pl.ds(2 * (1 - core), 2)]
    remote(got, got, dap_sem.at[0], dap_sem.at[1], sibling).wait_recv()
    mine_b.wait()
    for shift in (1, N3, 2):
        b_scatter(shift).start()
    b_out[core, :, y, z] = b_mid[y]

    half = ((0, N16), (0, N16), (0, N8), (N8, N8))
    shifts = (0, 0, -1, 1)
    landed = (-1, 1, -2, 2)

    def a_gather(kind, shift):
        c0, n = half[kind]
        ref = a_out.at[pl.ds(c0, n), ypos(shift)]
        return remote(ref, ref, ag_send.at[kind], ag_recv.at[kind], ypeer(1 if kind % 2 == 0 else -1))

    def b_gather(kind, shift):
        c0, n = half[kind]
        ref = b_out.at[core, pl.ds(c0, n), :, zpos(shift)]
        return remote(ref, ref, bg_send.at[kind], bg_recv.at[kind], zpeer(1 if kind % 2 == 0 else -1))

    def share(slot, which, shift, kind):
        c0, n = half[kind]
        ref = b_out.at[which, pl.ds(c0, n), :, zpos(shift)]
        return remote(ref, ref, sib_send.at[slot], sib_recv.at[slot], sibling)

    shared = ((0, 0), (-1, 0), (1, 0), (-2, 2), (2, N3))
    for shift in (1, N3, 2):
        a_scattered(shift).wait_recv()
    mine_a.wait()
    a_gather(0, 0).start()
    a_gather(1, 0).start()
    for shift in (1, N3, 2):
        b_scattered(shift).wait_recv()
    b_gather(0, 0).start()
    b_gather(1, 0).start()
    share(0, core, *shared[0]).start()
    for kind in (0, 1):
        a_gather(kind, landed[kind]).wait_recv()
        a_gather(kind + 2, shifts[kind + 2]).start()
        b_gather(kind, landed[kind]).wait_recv()
        b_gather(kind + 2, shifts[kind + 2]).start()
        share(kind + 1, core, *shared[kind + 1]).start()
    for kind in (2, N3):
        b_gather(kind, landed[kind]).wait_recv()
        share(kind + 1, core, *shared[kind + 1]).start()
    for kind in (2, N3):
        a_gather(kind, landed[kind]).wait_recv()
    for slot in range(N5):
        share(slot, 1 - core, *shared[slot]).wait_recv()
    to_sib.wait_send()
    m_store.wait()
    other_cols = m_out.at[:, :, pl.ds(pl.multiple_of((1 - core) * N256, N256), N256)]
    remote(other_cols, other_cols, m_sem.at[0], m_sem.at[1], sibling).wait_recv()
    m_far.wait_send()
    for shift in (1, N3, 2):
        a_scatter(shift).wait_send()
        b_scatter(shift).wait_send()
    for kind in range(N4):
        a_gather(kind, shifts[kind]).wait_send()
        b_gather(kind, shifts[kind]).wait_send()
    for slot in range(N5):
        share(slot, core, *shared[slot]).wait_send()


def exchange(a_loc, b_loc, msa_t):
    dma = pltpu.SemaphoreType.DMA
    return pl.pallas_call(
        exchange_kernel,
        in_specs=[pl.BlockSpec(memory_space=pl.ANY)] * N3,
        out_specs=(pl.BlockSpec(memory_space=pltpu.VMEM),) * 2 + (pl.BlockSpec(memory_space=pl.ANY),),
        out_shape=(jax.ShapeDtypeStruct((N16, N4, N4, N32, N128), jnp.bfloat16), jax.ShapeDtypeStruct((2, N16, N4, N4, N32, N128), jnp.bfloat16), jax.ShapeDtypeStruct((N16, N64, N512), jnp.bfloat16)),
        scratch_shapes=[pltpu.VMEM((N4, N16, N32, N128), jnp.bfloat16), pltpu.VMEM((N16, N64, N256), jnp.bfloat16), dma((N4,)), dma((2,)), dma((2,))] + [dma((N4,))] * N8 + [dma((N5,))] * 2,
        compiler_params=pltpu.CompilerParams(collective_id=2, has_side_effects=True),
        name='exchange',
    )(a_loc, b_loc, msa_t)


def pair_kernel(a_ref, b_ref, w_ref, out0, out1, out2, out3, at_f32, at, outer):
    x = lax.rem(lax.axis_index('seq'), N4)
    def transpose_a(c, _):
        for sb in range(N4):
            blk = a_ref[c, sb * N128:sb * N128 + N128, :].astype(jnp.float32).T
            at_f32[sb, pl.ds(pl.multiple_of(c * STRIDE, N8), N64), :] = blk[:N64]
            at_f32[sb, pl.ds(pl.multiple_of((c + N16) * STRIDE, N8), N64), :] = blk[N64:]
        return 0

    lax.fori_loop(0, N16, transpose_a, 0)

    def regroup(i, _):
        for sb in range(N4):
            rows = at_f32[sb, pl.ds(i, N32, stride=STRIDE), :]
            at[pl.ds(pl.multiple_of(i * N32, N32), N32), sb * N128:sb * N128 + N128] = rows.astype(jnp.bfloat16)
        return 0

    lax.fori_loop(0, N64, regroup, 0, unroll=2)

    def products(dp, _):
        rhs = jnp.concatenate([b_ref[2 * dp], b_ref[2 * dp + 1]], axis=1)
        for mc in range(N4):
            prod = jnp.dot(at[mc * N512:mc * N512 + N512, :], rhs, preferred_element_type=jnp.float32).astype(jnp.bfloat16)
            for i in range(N16):
                for dd in range(2):
                    row = pl.multiple_of((2 * dp + dd) * N32, N32)
                    lane = (i % 2) * N128
                    outer[mc * N8 + i // 2, pl.ds(row, N32), lane:lane + N128] = prod[i * N32:i * N32 + N32, dd * N128:dd * N128 + N128]
        return 0

    lax.fori_loop(0, N16, products, 0)
    w = w_ref[...]

    for dist, out_ref in enumerate((out0, out1, out2, out3)):
        first = lax.rem(x + dist, N4) * N8

        def combine(k, _):
            res = jnp.dot(w, outer[first + k], preferred_element_type=jnp.float32)
            out_ref[2 * k] = res[:, :N128].T.astype(jnp.bfloat16)
            out_ref[2 * k + 1] = res[:, N128:].T.astype(jnp.bfloat16)
            return 0

        lax.fori_loop(0, N8, combine, 0, unroll=N4)


def pair_partial(a_full, b_full, w2):
    return pl.pallas_call(
        pair_kernel,
        out_shape=(jax.ShapeDtypeStruct((N16, N128, N128), jnp.bfloat16),) * N4,
        scratch_shapes=[pltpu.VMEM((N4, N32 * STRIDE, N128), jnp.float32), pltpu.VMEM((2048, N512), jnp.bfloat16), pltpu.VMEM((N32, 1024, N256), jnp.bfloat16)],
        cost_estimate=pl.CostEstimate(flops=12_000_000_000, bytes_accessed=8_000_000, transcendentals=0),
        name='pair_partial',
    )(a_full.reshape(N16, N512, N128), b_full.reshape(N32, N512, N128), w2)


AXES = ((2, 1, 0), (1, 0, 2), (0, 2, 1))
OTHER = ((1, 2), (0, 1), (0, 2))
ROW0 = (0, N5, 10)
HALF = ((0, N3), (N3, 2))
COLS = ((0, 48), (48, 40), (88, 40))
COL_LOW = (24, 24, N16)
STRIDES = (N16, N4, 1)


def coords():
    seq = lax.axis_index('seq')
    return seq // N16, lax.rem(seq // N4, N4), lax.rem(seq, N4)


def gather_kernel(t_ref, *refs):
    own, near = refs[0:N3], refs[N3:6]
    last_row, send_sem, recv_sem, near_send, near_recv, row_send, row_recv, own_sem = refs[6:]
    seq = lax.axis_index('seq')
    onward = 1 - 2 * lax.axis_index('dap')
    me = coords()

    def at(axis, step):
        return lax.rem(me[axis] + step + N4, N4)

    def peer(axis, step):
        return {'seq': seq + (at(axis, step) - me[axis]) * STRIDES[axis]}

    barrier = pltpu.get_barrier_semaphore()
    for axis in range(N3):
        for step in (1, -1):
            pl.semaphore_signal(barrier, inc=1, device_id=peer(axis, step), device_id_type=MESH)
    pl.semaphore_wait(barrier, 6)

    def index(part, phase, shift, axes):
        idx = []
        for axis in axes:
            if axis in AXES[part][:phase]:
                idx.append(pl.ds(0, N4))
            elif axis == AXES[part][phase]:
                idx.append(pl.ds(at(axis, shift), 1))
            else:
                idx.append(pl.ds(me[axis], 1))
        return tuple(idx)

    def piece(total, low, kind):
        return ((0, total), (0, total), (0, low), (low, total - low))[kind]

    def copy(c, part, phase, kind, shift):
        to = peer(AXES[part][phase], 1 if kind % 2 == 0 else -1)
        if c == 2:
            lo, n = piece(COLS[part][1], COL_LOW[part], kind)
            ref = last_row.at[index(part, phase, shift, (0, 1, 2)) + (pl.ds(COLS[part][0] + lo, n),)]
            src = ref
            if phase == 0 and shift == 0:
                src = t_ref.at[:, :, pl.ds(15, 1), pl.ds(COLS[part][0] + lo, n)]
            sems = (row_send.at[part, phase, kind], row_recv.at[part, phase, kind])
        else:
            base, rows = HALF[c]
            lo, n = piece(rows, 2 - part % 2 if c == 0 else 1, kind)
            ref = own[part].at[index(part, phase, shift, OTHER[part]) + (pl.ds(base + lo, n),)]
            src = ref
            if phase == 0 and shift == 0:
                src = t_ref.at[:, :, pl.ds(ROW0[part] + base + lo, n)]
            sems = (send_sem.at[c, part, phase, kind], recv_sem.at[c, part, phase, kind])
        return pltpu.make_async_remote_copy(src_ref=src, dst_ref=ref, send_sem=sems[0], recv_sem=sems[1], device_id=to, device_id_type=MESH)

    sent = (0, 0, -1, 1)
    got = (-1, 1, -2, 2)

    def last_copy(c, part):
        to = peer(AXES[part][2], onward)
        idx = (slice(None), slice(None), pl.ds(*HALF[c]))
        return pltpu.make_async_remote_copy(src_ref=own[part].at[idx], dst_ref=near[part].at[idx], send_sem=near_send.at[c, part], recv_sem=near_recv.at[c, part], device_id=to, device_id_type=MESH)

    mains = [(c, p) for c in range(2) for p in range(N3)]
    order = [(c, p) for c in range(N3) for p in range(N3)]
    for c, p in order:
        copy(c, p, 0, 0, 0).start()
        copy(c, p, 0, 1, 0).start()
    local = []
    for p in range(N3):
        dst = own[p].at[tuple(pl.ds(me[axis], 1) for axis in OTHER[p])]
        local.append(pltpu.make_async_copy(t_ref.at[:, :, pl.ds(ROW0[p], N5)], dst, own_sem.at[p]))
    local.append(pltpu.make_async_copy(t_ref.at[:, :, pl.ds(15, 1)], last_row.at[tuple(pl.ds(me[axis], 1) for axis in range(N3))], own_sem.at[N3]))
    for item in local:
        item.start()
    for item in local:
        item.wait()
    for phase in range(N3):
        active = [(c, p) for c, p in order if phase < 2 or c == 2]
        for c, p in active:
            for kind in (0, 1):
                copy(c, p, phase, kind, got[kind]).wait_recv()
                copy(c, p, phase, kind + 2, sent[kind + 2]).start()
        for c, p in active:
            for kind in (2, N3):
                copy(c, p, phase, kind, got[kind]).wait_recv()
            if phase == 0 or (phase == 1 and c == 2):
                copy(c, p, phase + 1, 0, 0).start()
                copy(c, p, phase + 1, 1, 0).start()
            elif phase == 1:
                last_copy(c, p).start()
    for c, p in mains:
        last_copy(c, p).wait_recv()
    for c, p in order:
        for phase in range(N3 if c == 2 else 2):
            for kind in range(N4):
                copy(c, p, phase, kind, sent[kind]).wait_send()
        if c < 2:
            last_copy(c, p).wait_send()


def gather(tile):
    parts = [jax.ShapeDtypeStruct((N4, N4, N5, N128, N128), jnp.bfloat16) for _ in range(6)]
    dma = pltpu.SemaphoreType.DMA
    res = pl.pallas_call(
        gather_kernel,
        in_specs=[pl.BlockSpec(memory_space=pltpu.VMEM)],
        out_specs=[pl.BlockSpec(memory_space=pl.ANY)] * 7,
        out_shape=parts + [jax.ShapeDtypeStruct((N4, N4, N4, N128, N128), jnp.bfloat16)],
        scratch_shapes=[dma((2, N3, 2, N4)), dma((2, N3, 2, N4)), dma((2, N3)), dma((2, N3)), dma((N3, N3, N4)), dma((N3, N3, N4)), dma((N4,))],
        compiler_params=pltpu.CompilerParams(collective_id=1, has_side_effects=True),
        name='gather_tiles',
    )(tile.reshape(1, 1, N16, N128, N128))
    return res[0:N3], res[N3:6], res[6]


SLOTS = 12
AHEAD = N8


def update_kernel(items, n_src, n_prev, z_ref, inv_ref, b_ref, *refs):
    srcs = refs[:n_src]
    out_ref, buf, gbuf, in_sem, out_sem = refs[n_src + n_prev:]
    me = coords()
    bias = b_ref[...]
    onward = 1 - 2 * lax.axis_index('dap')

    def place(item):
        part, shift, k = item[0], item[1], item[2]
        if part == N3:
            return k, None, None
        pos = lax.rem(me[AXES[part][2]] + shift * onward + N4, N4)
        return ((pos, None, k), (k, None, pos), (k, pos, None))[part]

    def rows_of(item):
        return N4 if item[0] == N3 else N5

    def z_slices(ref, item, slot):
        part = item[0]
        zd, yd, xd = place(item)
        if part == N3:
            return [(ref.at[zd * N4 + x, 15], buf.at[slot, :, x]) for x in range(N4)]
        if part == 2:
            return [(ref.at[pl.ds(zd * N4, N4), pl.ds(ROW0[part], N5), yd], buf.at[slot])]
        return [(ref.at[zd * N4 + xd, ROW0[part] + r], buf.at[slot, :, r]) for r in range(N5)]

    def g_slices(item, slot):
        part, _, k, src = item
        ref = srcs[src]
        if part == N3:
            return [(ref.at[k, :, x], gbuf.at[slot, :, x]) for x in range(N4)]
        return [(ref.at[:, k] if part == 0 else ref.at[k], gbuf.at[slot])]

    def start_in(i):
        slot = i % SLOTS
        for src, dst in z_slices(z_ref, items[i], slot):
            pltpu.make_async_copy(src, dst, in_sem.at[slot, 0]).start()
        for src, dst in g_slices(items[i], slot):
            pltpu.make_async_copy(src, dst, in_sem.at[slot, 1]).start()

    def wait_in(i):
        slot = i % SLOTS
        n = rows_of(items[i])
        zb, gb = buf.at[slot, :, pl.ds(0, n)], gbuf.at[slot, :, pl.ds(0, n)]
        pltpu.make_async_copy(zb, zb, in_sem.at[slot, 0]).wait()
        pltpu.make_async_copy(gb, gb, in_sem.at[slot, 1]).wait()

    def start_out(i):
        slot = i % SLOTS
        for dst, src in z_slices(out_ref, items[i], slot):
            pltpu.make_async_copy(src, dst, out_sem.at[slot]).start()

    def wait_out(i):
        slot = i % SLOTS
        zb = buf.at[slot, :, pl.ds(0, rows_of(items[i]))]
        pltpu.make_async_copy(zb, zb, out_sem.at[slot]).wait()

    def compute(i):
        slot = i % SLOTS
        item = items[i]
        part = item[0]
        zd, yd, xd = place(item)

        offs = tuple(x * N16 for x in range(N4)) if part == N3 else tuple(range(N5))

        def body(q, _):
            lane, yq = zd * N64, q
            if part == N3:
                lane = lane + 15
            elif part == 2:
                lane, yq = lane + q * N16 + ROW0[part], yd
            else:
                lane = lane + xd * N16 + ROW0[part]
            inv = inv_ref[lane // N128, pl.ds(pl.multiple_of(yq * N128, N128), N128), :]
            inv = pltpu.roll(inv, lax.rem(N256 - lane, N128), 1)
            for r, off in enumerate(offs):
                seg = gbuf[slot, q, r].astype(jnp.float32)
                buf[slot, q, r] = buf[slot, q, r] + (seg + bias) * inv[:, off:off + 1]
            return 0

        lax.fori_loop(0, N4, body, 0)

    n = len(items)
    for i in range(min(AHEAD, n)):
        start_in(i)
    for i in range(n):
        j = i + AHEAD
        if j < n:
            if j >= SLOTS:
                wait_out(j - SLOTS)
            start_in(j)
        wait_in(i)
        compute(i)
        start_out(i)
    for i in range(max(0, n - SLOTS), n):
        wait_out(i)


def update(name, items, pair5, inv2, bias, srcs, prev):
    any_spec = pl.BlockSpec(memory_space=pl.ANY)
    vmem_spec = pl.BlockSpec(memory_space=pltpu.VMEM)
    args = [pair5, inv2, bias] + srcs + ([] if prev is None else [prev])
    blocks = len(items) * N16
    return pl.pallas_call(
        functools.partial(update_kernel, items, len(srcs), len(args) - N3 - len(srcs)),
        in_specs=[any_spec, vmem_spec, vmem_spec] + [any_spec] * (len(args) - N3),
        out_specs=any_spec,
        out_shape=jax.ShapeDtypeStruct(pair5.shape, jnp.float32),
        scratch_shapes=[pltpu.VMEM((SLOTS, N4, N5, N128, N128), jnp.float32), pltpu.VMEM((SLOTS, N4, N5, N128, N128), jnp.bfloat16), pltpu.SemaphoreType.DMA((SLOTS, 2)), pltpu.SemaphoreType.DMA((SLOTS,))],
        input_output_aliases={} if prev is None else {len(args) - 1: 0},
        cost_estimate=pl.CostEstimate(flops=blocks * 40_000_000, bytes_accessed=blocks * 163840, transcendentals=0),
        name=name,
    )(*args)


def ring(axis, step, mirror):
    out = []
    for i in range(N64):
        pos = i // STRIDES[axis] % N4
        for core in range(2):
            to = i + ((pos + step * (1 - 2 * core * mirror)) % N4 - pos) * STRIDES[axis]
            out.append((2 * i + core, 2 * to + core))
    return out


def gather_and_update(tile, pair_rows, inv2, bias):
    own, near, last_row = gather(tile)
    pair5 = pair_rows.reshape(N16, N16, N4, N128, N128)
    send = lambda x, p, step: lax.ppermute(x, ('seq', 'dap'), ring(AXES[p][2], step, 1))
    items = lambda shift, base: [(p, shift, k, base + p) for p in range(N3) for k in range(N4)]
    ahead = [send(own[p], p, -1) for p in range(N3)]
    first = [(N3, 0, k, N3) for k in range(N4)] + items(0, 0)
    out = update('update_own', first, pair5, inv2, bias, list(own) + [last_row], None)
    near, out = lax.optimization_barrier((near, out))
    far = [send(near[p], p, 1) for p in range(N3)]
    out = update('update_behind', items(-1, 0), pair5, inv2, bias, list(near), out)
    out = update('update_ahead', items(1, 0), pair5, inv2, bias, ahead, out)
    out = update('update_far', items(2, 0), pair5, inv2, bias, far, out)
    return out.reshape(pair_rows.shape)


def solution(mesh):
    rep = P()
    in_specs = (P(('data', 'seq'), 'dap', None), P('data', None), P(('data', 'dap'), None, None)) + (rep,) * N8
    out_specs = (P(('data', 'dap'), None, None), P(('data', 'seq', 'dap'), None, None))

    def local_fn(msa, mask, pair_rows, ln_gamma, ln_beta, w_left, b_left, w_right, b_right, w_out, b_out):
        dap_idx = lax.axis_index('dap')
        msa_t = jnp.swapaxes(msa, 1, 2)
        rows = jnp.stack([ln_gamma, ln_beta, jnp.concatenate([b_left, b_right])]).astype(jnp.float32)
        vecs = jnp.pad(rows, ((0, N5), (0, N64)))
        a_loc, b_loc = project(msa_t, mask, vecs, w_left.T, w_right.T)
        a_full, b_full, m_full = exchange(a_loc, b_loc, msa_t)
        msa_out = jnp.swapaxes(m_full, 1, 2)
        w2 = w_out.reshape(N32, N32, N128).transpose(2, 1, 0).reshape(N128, 1024)
        terms = pair_partial(a_full, b_full, w2)
        move = lambda v, step, mirror: lax.ppermute(v, ('seq', 'dap'), ring(2, step, mirror))
        relay = move(terms[2], 1, 1)
        after, before = move(terms[1], 1, 0), move(terms[N3], -1, 0)
        parts = [terms[0], after, before, move(relay, 1, 1)]
        total = sum(v.astype(jnp.float32) for v in parts).astype(jnp.bfloat16)

        mask_bf16 = mask.astype(jnp.bfloat16)
        mask_rows = lax.dynamic_slice_in_dim(mask_bf16, dap_idx * N256, N256, axis=1)
        count_t = jnp.einsum('sj,sti->tji', mask_bf16, mask_rows.reshape(2048, 2, N128), preferred_element_type=jnp.float32)
        inv2 = 1.0 / (1e-3 + count_t)
        bias = b_out.astype(jnp.float32).reshape(1, N128)

        total, inv2, bias = lax.optimization_barrier((total, inv2, bias))
        out = gather_and_update(total, pair_rows, inv2, bias)
        return out, msa_out

    return jax.shard_map(local_fn, mesh=mesh, in_specs=in_specs, out_specs=out_specs, check_vma=False)
```

```python
import functools

import jax
import jax.numpy as jnp
from jax import lax
from jax.experimental import pallas as pl
from jax.experimental.pallas import tpu as pltpu
from jax.sharding import PartitionSpec as P


N3, N4, N5, N8, N16, N32, N64, N128, N256, N512 = 3, 4, 5, 8, 16, 32, 64, 128, 256, 512
STRIDE = 72


def project_kernel(m_ref, mask_hbm, vec_ref, wl_ref, wr_ref, a_ref, b_ref, scr, mask_i32, sem):
    row = pl.multiple_of(lax.axis_index('seq') * N32, N32)
    lane = pl.multiple_of(lax.axis_index('dap') * N256, N256)
    load = pltpu.make_async_copy(mask_hbm.at[pl.ds(row, N32), pl.ds(lane, N256)], mask_i32, sem)
    load.start()
    vecs = vec_ref[...].T
    gamma, beta, bias = vecs[:N64, 0:1], vecs[:N64, 1:2], vecs[:N64, 2:N3]
    w = jnp.concatenate([wl_ref[...], wr_ref[...]], axis=0)
    load.wait()
    for s in range(N32):
        x = m_ref[s].astype(jnp.float32)
        cen = x - jnp.mean(x, axis=0, keepdims=True)
        var = jnp.mean(cen * cen, axis=0, keepdims=True)
        normed = (cen * lax.rsqrt(var + 1e-5) * gamma + beta).astype(jnp.bfloat16)
        out = (jnp.dot(w, normed, preferred_element_type=jnp.float32) + bias) * mask_i32[s:s + 1, :].astype(jnp.float32)
        for t in range(2):
            scr[t, s * STRIDE:s * STRIDE + N64, :] = out[:, t * N128:t * N128 + N128]
    low = lax.broadcasted_iota(jnp.int32, (N32, N128), 1) < N64
    for t in range(2):
        for c in range(N16):
            lo = scr[t, pl.ds(c, N32, stride=STRIDE), :]
            hi = scr[t, pl.ds(N16 + c, N32, stride=STRIDE), :]
            a_ref[2 * t, c] = jnp.where(low, lo, pltpu.roll(hi, N64, 1)).astype(jnp.bfloat16)
            a_ref[2 * t + 1, c] = jnp.where(low, pltpu.roll(lo, N64, 1), hi).astype(jnp.bfloat16)
        for d in range(N32):
            b_ref[d // N16, t, d % N16] = scr[t, pl.ds(N32 + d, N32, stride=STRIDE), :].astype(jnp.bfloat16)


def project(msa_t, mask, vecs, w_l, w_r):
    vmem_spec = pl.BlockSpec(memory_space=pltpu.VMEM)
    return pl.pallas_call(
        project_kernel,
        in_specs=[vmem_spec, pl.BlockSpec(memory_space=pl.ANY), vmem_spec, vmem_spec, vmem_spec],
        out_shape=(jax.ShapeDtypeStruct((N4, N16, N32, N128), jnp.bfloat16), jax.ShapeDtypeStruct((2, 2, N16, N32, N128), jnp.bfloat16)),
        scratch_shapes=[pltpu.VMEM((2, N32 * STRIDE, N128), jnp.float32), pltpu.VMEM((N32, N256), jnp.int32), pltpu.SemaphoreType.DMA],
        name='project',
    )(msa_t, mask, vecs, w_l, w_r)


MESH = pl.DeviceIdType.MESH


def exchange_kernel(a_in, b_in, m_in, a_out, b_out, m_out, b_mid, m_mid, m_sem, dap_sem, loc_sem, aa_send, aa_recv, bb_send, bb_recv, ag_send, ag_recv, bg_send, bg_recv, sib_send, sib_recv):
    seq = lax.axis_index('seq')
    core = lax.axis_index('dap')
    z, y = seq // N16, lax.rem(seq // N4, N4)

    def zpos(step):
        return lax.rem(z + step + N4, N4)

    def ypos(step):
        return lax.rem(y + step + N4, N4)

    def zpeer(step):
        return {'seq': seq + (zpos(step) - z) * N16}

    def ypeer(step):
        return {'seq': seq + (ypos(step) - y) * N4}

    sibling = {'dap': 1 - core}
    barrier = pltpu.get_barrier_semaphore()
    for peer in [zpeer(i) for i in (1, 2, N3)] + [ypeer(i) for i in (1, 2, N3)] + [sibling]:
        pl.semaphore_signal(barrier, inc=1, device_id=peer, device_id_type=MESH)
    pl.semaphore_wait(barrier, 7)

    def remote(src, dst, ssem, rsem, peer):
        return pltpu.make_async_remote_copy(src_ref=src, dst_ref=dst, send_sem=ssem, recv_sem=rsem, device_id=peer, device_id_type=MESH)

    to_sib = remote(b_in.at[1 - core], b_mid.at[pl.ds(2 * core, 2)], dap_sem.at[0], dap_sem.at[1], sibling)
    to_sib.start()
    mine_b = pltpu.make_async_copy(b_in.at[core], b_mid.at[pl.ds(2 * core, 2)], loc_sem.at[0])
    mine_b.start()
    mine_a = pltpu.make_async_copy(a_in.at[z], a_out.at[:, y, z], loc_sem.at[1])
    mine_a.start()

    def a_scatter(shift):
        return remote(a_in.at[zpos(shift)], a_out.at[:, y, z], aa_send.at[shift], aa_recv.at[shift], zpeer(shift))

    def a_scattered(shift):
        ref = a_out.at[:, y, zpos(-shift)]
        return remote(ref, ref, aa_send.at[shift], aa_recv.at[shift], zpeer(shift))

    def b_scatter(shift):
        return remote(b_mid.at[ypos(shift)], b_out.at[core, :, y, z], bb_send.at[shift], bb_recv.at[shift], ypeer(shift))

    def b_scattered(shift):
        ref = b_out.at[core, :, ypos(-shift), z]
        return remote(ref, ref, bb_send.at[shift], bb_recv.at[shift], ypeer(shift))

    for shift in (1, N3, 2):
        a_scatter(shift).start()
    half_cols = m_out.at[:, :, pl.ds(pl.multiple_of(core * N256, N256), N256)]
    m_far = remote(m_in.at[pl.ds(N16 * (1 - core), N16)], half_cols, m_sem.at[0], m_sem.at[1], sibling)
    m_far.start()
    m_load = pltpu.make_async_copy(m_in.at[pl.ds(N16 * core, N16)], m_mid, m_sem.at[2])
    m_load.start()
    m_load.wait()
    m_store = pltpu.make_async_copy(m_mid, half_cols, m_sem.at[N3])
    m_store.start()
    got = b_mid.at[pl.ds(2 * (1 - core), 2)]
    remote(got, got, dap_sem.at[0], dap_sem.at[1], sibling).wait_recv()
    mine_b.wait()
    for shift in (1, N3, 2):
        b_scatter(shift).start()
    b_out[core, :, y, z] = b_mid[y]

    half = ((0, N16), (0, N16), (0, N8), (N8, N8))
    shifts = (0, 0, -1, 1)
    landed = (-1, 1, -2, 2)

    def a_gather(kind, shift):
        c0, n = half[kind]
        ref = a_out.at[pl.ds(c0, n), ypos(shift)]
        return remote(ref, ref, ag_send.at[kind], ag_recv.at[kind], ypeer(1 if kind % 2 == 0 else -1))

    def b_gather(kind, shift):
        c0, n = half[kind]
        ref = b_out.at[core, pl.ds(c0, n), :, zpos(shift)]
        return remote(ref, ref, bg_send.at[kind], bg_recv.at[kind], zpeer(1 if kind % 2 == 0 else -1))

    def share(slot, which, shift, kind):
        c0, n = half[kind]
        ref = b_out.at[which, pl.ds(c0, n), :, zpos(shift)]
        return remote(ref, ref, sib_send.at[slot], sib_recv.at[slot], sibling)

    shared = ((0, 0), (-1, 0), (1, 0), (-2, 2), (2, N3))
    for shift in (1, N3, 2):
        a_scattered(shift).wait_recv()
    mine_a.wait()
    a_gather(0, 0).start()
    a_gather(1, 0).start()
    for shift in (1, N3, 2):
        b_scattered(shift).wait_recv()
    b_gather(0, 0).start()
    b_gather(1, 0).start()
    share(0, core, *shared[0]).start()
    for kind in (0, 1):
        a_gather(kind, landed[kind]).wait_recv()
        a_gather(kind + 2, shifts[kind + 2]).start()
        b_gather(kind, landed[kind]).wait_recv()
        b_gather(kind + 2, shifts[kind + 2]).start()
        share(kind + 1, core, *shared[kind + 1]).start()
    for kind in (2, N3):
        b_gather(kind, landed[kind]).wait_recv()
        share(kind + 1, core, *shared[kind + 1]).start()
    for kind in (2, N3):
        a_gather(kind, landed[kind]).wait_recv()
    for slot in range(N5):
        share(slot, 1 - core, *shared[slot]).wait_recv()
    to_sib.wait_send()
    m_store.wait()
    other_cols = m_out.at[:, :, pl.ds(pl.multiple_of((1 - core) * N256, N256), N256)]
    remote(other_cols, other_cols, m_sem.at[0], m_sem.at[1], sibling).wait_recv()
    m_far.wait_send()
    for shift in (1, N3, 2):
        a_scatter(shift).wait_send()
        b_scatter(shift).wait_send()
    for kind in range(N4):
        a_gather(kind, shifts[kind]).wait_send()
        b_gather(kind, shifts[kind]).wait_send()
    for slot in range(N5):
        share(slot, core, *shared[slot]).wait_send()


def exchange(a_loc, b_loc, msa_t):
    dma = pltpu.SemaphoreType.DMA
    return pl.pallas_call(
        exchange_kernel,
        in_specs=[pl.BlockSpec(memory_space=pl.ANY)] * N3,
        out_specs=(pl.BlockSpec(memory_space=pltpu.VMEM),) * 2 + (pl.BlockSpec(memory_space=pl.ANY),),
        out_shape=(jax.ShapeDtypeStruct((N16, N4, N4, N32, N128), jnp.bfloat16), jax.ShapeDtypeStruct((2, N16, N4, N4, N32, N128), jnp.bfloat16), jax.ShapeDtypeStruct((N16, N64, N512), jnp.bfloat16)),
        scratch_shapes=[pltpu.VMEM((N4, N16, N32, N128), jnp.bfloat16), pltpu.VMEM((N16, N64, N256), jnp.bfloat16), dma((N4,)), dma((2,)), dma((2,))] + [dma((N4,))] * N8 + [dma((N5,))] * 2,
        compiler_params=pltpu.CompilerParams(collective_id=2, has_side_effects=True),
        name='exchange',
    )(a_loc, b_loc, msa_t)


def pair_kernel(a_ref, b_ref, w_ref, out0, out1, out2, out3, at_f32, at, outer):
    x = lax.rem(lax.axis_index('seq'), N4)
    def transpose_a(c, _):
        for sb in range(N4):
            blk = a_ref[c, sb * N128:sb * N128 + N128, :].astype(jnp.float32).T
            at_f32[sb, pl.ds(pl.multiple_of(c * STRIDE, N8), N64), :] = blk[:N64]
            at_f32[sb, pl.ds(pl.multiple_of((c + N16) * STRIDE, N8), N64), :] = blk[N64:]
        return 0

    lax.fori_loop(0, N16, transpose_a, 0)

    def regroup(i, _):
        for sb in range(N4):
            rows = at_f32[sb, pl.ds(i, N32, stride=STRIDE), :]
            at[pl.ds(pl.multiple_of(i * N32, N32), N32), sb * N128:sb * N128 + N128] = rows.astype(jnp.bfloat16)
        return 0

    lax.fori_loop(0, N64, regroup, 0, unroll=2)

    def products(dp, _):
        rhs = jnp.concatenate([b_ref[2 * dp], b_ref[2 * dp + 1]], axis=1)
        for mc in range(N4):
            prod = jnp.dot(at[mc * N512:mc * N512 + N512, :], rhs, preferred_element_type=jnp.float32).astype(jnp.bfloat16)
            for i in range(N16):
                for dd in range(2):
                    row = pl.multiple_of((2 * dp + dd) * N32, N32)
                    lane = (i % 2) * N128
                    outer[mc * N8 + i // 2, pl.ds(row, N32), lane:lane + N128] = prod[i * N32:i * N32 + N32, dd * N128:dd * N128 + N128]
        return 0

    lax.fori_loop(0, N16, products, 0)
    w = w_ref[...]

    for dist, out_ref in enumerate((out0, out1, out2, out3)):
        first = lax.rem(x + dist, N4) * N8

        def combine(k, _):
            res = jnp.dot(w, outer[first + k], preferred_element_type=jnp.float32)
            out_ref[2 * k] = res[:, :N128].T.astype(jnp.bfloat16)
            out_ref[2 * k + 1] = res[:, N128:].T.astype(jnp.bfloat16)
            return 0

        lax.fori_loop(0, N8, combine, 0, unroll=N4)


def pair_partial(a_full, b_full, w2):
    return pl.pallas_call(
        pair_kernel,
        out_shape=(jax.ShapeDtypeStruct((N16, N128, N128), jnp.bfloat16),) * N4,
        scratch_shapes=[pltpu.VMEM((N4, N32 * STRIDE, N128), jnp.float32), pltpu.VMEM((2048, N512), jnp.bfloat16), pltpu.VMEM((N32, 1024, N256), jnp.bfloat16)],
        cost_estimate=pl.CostEstimate(flops=12_000_000_000, bytes_accessed=8_000_000, transcendentals=0),
        name='pair_partial',
    )(a_full.reshape(N16, N512, N128), b_full.reshape(N32, N512, N128), w2)


AXES = ((2, 1, 0), (1, 0, 2), (0, 2, 1))
OTHER = ((1, 2), (0, 1), (0, 2))
ROW0 = (0, N5, 10)
HALF = ((0, N3), (N3, 2))
COLS = ((0, 48), (48, 40), (88, 40))
COL_LOW = (24, 24, N16)
STRIDES = (N16, N4, 1)


def coords():
    seq = lax.axis_index('seq')
    return seq // N16, lax.rem(seq // N4, N4), lax.rem(seq, N4)


def gather_kernel(t_ref, *refs):
    own, near = refs[0:N3], refs[N3:6]
    last_row, send_sem, recv_sem, near_send, near_recv, row_send, row_recv, own_sem = refs[6:]
    seq = lax.axis_index('seq')
    onward = 1 - 2 * lax.axis_index('dap')
    me = coords()

    def at(axis, step):
        return lax.rem(me[axis] + step + N4, N4)

    def peer(axis, step):
        return {'seq': seq + (at(axis, step) - me[axis]) * STRIDES[axis]}

    barrier = pltpu.get_barrier_semaphore()
    for axis in range(N3):
        for step in (1, -1):
            pl.semaphore_signal(barrier, inc=1, device_id=peer(axis, step), device_id_type=MESH)
    pl.semaphore_wait(barrier, 6)

    def index(part, phase, shift, axes):
        idx = []
        for axis in axes:
            if axis in AXES[part][:phase]:
                idx.append(pl.ds(0, N4))
            elif axis == AXES[part][phase]:
                idx.append(pl.ds(at(axis, shift), 1))
            else:
                idx.append(pl.ds(me[axis], 1))
        return tuple(idx)

    def piece(total, low, kind):
        return ((0, total), (0, total), (0, low), (low, total - low))[kind]

    def copy(c, part, phase, kind, shift):
        to = peer(AXES[part][phase], 1 if kind % 2 == 0 else -1)
        if c == 2:
            lo, n = piece(COLS[part][1], COL_LOW[part], kind)
            ref = last_row.at[index(part, phase, shift, (0, 1, 2)) + (pl.ds(COLS[part][0] + lo, n),)]
            src = ref
            if phase == 0 and shift == 0:
                src = t_ref.at[:, :, pl.ds(15, 1), pl.ds(COLS[part][0] + lo, n)]
            sems = (row_send.at[part, phase, kind], row_recv.at[part, phase, kind])
        else:
            base, rows = HALF[c]
            lo, n = piece(rows, 2 - part % 2 if c == 0 else 1, kind)
            ref = own[part].at[index(part, phase, shift, OTHER[part]) + (pl.ds(base + lo, n),)]
            src = ref
            if phase == 0 and shift == 0:
                src = t_ref.at[:, :, pl.ds(ROW0[part] + base + lo, n)]
            sems = (send_sem.at[c, part, phase, kind], recv_sem.at[c, part, phase, kind])
        return pltpu.make_async_remote_copy(src_ref=src, dst_ref=ref, send_sem=sems[0], recv_sem=sems[1], device_id=to, device_id_type=MESH)

    sent = (0, 0, -1, 1)
    got = (-1, 1, -2, 2)

    def last_copy(c, part):
        to = peer(AXES[part][2], onward)
        idx = (slice(None), slice(None), pl.ds(*HALF[c]))
        return pltpu.make_async_remote_copy(src_ref=own[part].at[idx], dst_ref=near[part].at[idx], send_sem=near_send.at[c, part], recv_sem=near_recv.at[c, part], device_id=to, device_id_type=MESH)

    mains = [(c, p) for c in range(2) for p in range(N3)]
    order = [(c, p) for c in (2, 0, 1) for p in range(N3)]
    for c, p in order:
        copy(c, p, 0, 0, 0).start()
        copy(c, p, 0, 1, 0).start()
    local = []
    for p in range(N3):
        dst = own[p].at[tuple(pl.ds(me[axis], 1) for axis in OTHER[p])]
        local.append(pltpu.make_async_copy(t_ref.at[:, :, pl.ds(ROW0[p], N5)], dst, own_sem.at[p]))
    local.append(pltpu.make_async_copy(t_ref.at[:, :, pl.ds(15, 1)], last_row.at[tuple(pl.ds(me[axis], 1) for axis in range(N3))], own_sem.at[N3]))
    for item in local:
        item.start()
    for item in local:
        item.wait()
    for phase in range(N3):
        active = [(c, p) for c, p in order if phase < 2 or c == 2]
        for c, p in active:
            for kind in (0, 1):
                copy(c, p, phase, kind, got[kind]).wait_recv()
                copy(c, p, phase, kind + 2, sent[kind + 2]).start()
        for c, p in active:
            for kind in (2, N3):
                copy(c, p, phase, kind, got[kind]).wait_recv()
            if phase == 0 or (phase == 1 and c == 2):
                copy(c, p, phase + 1, 0, 0).start()
                copy(c, p, phase + 1, 1, 0).start()
            elif phase == 1:
                last_copy(c, p).start()
    for c, p in mains:
        last_copy(c, p).wait_recv()
    for c, p in order:
        for phase in range(N3 if c == 2 else 2):
            for kind in range(N4):
                copy(c, p, phase, kind, sent[kind]).wait_send()
        if c < 2:
            last_copy(c, p).wait_send()


def gather(tile):
    parts = [jax.ShapeDtypeStruct((N4, N4, N5, N128, N128), jnp.bfloat16) for _ in range(6)]
    dma = pltpu.SemaphoreType.DMA
    res = pl.pallas_call(
        gather_kernel,
        in_specs=[pl.BlockSpec(memory_space=pltpu.VMEM)],
        out_specs=[pl.BlockSpec(memory_space=pl.ANY)] * 7,
        out_shape=parts + [jax.ShapeDtypeStruct((N4, N4, N4, N128, N128), jnp.bfloat16)],
        scratch_shapes=[dma((2, N3, 2, N4)), dma((2, N3, 2, N4)), dma((2, N3)), dma((2, N3)), dma((N3, N3, N4)), dma((N3, N3, N4)), dma((N4,))],
        compiler_params=pltpu.CompilerParams(collective_id=1, has_side_effects=True),
        name='gather_tiles',
    )(tile.reshape(1, 1, N16, N128, N128))
    return res[0:N3], res[N3:6], res[6]


SLOTS = 12
AHEAD = N8


def update_kernel(items, n_src, n_prev, z_ref, inv_ref, b_ref, *refs):
    srcs = refs[:n_src]
    out_ref, buf, gbuf, in_sem, out_sem = refs[n_src + n_prev:]
    me = coords()
    bias = b_ref[...]
    onward = 1 - 2 * lax.axis_index('dap')

    def place(item):
        part, shift, k = item[0], item[1], item[2]
        if part == N3:
            return k, None, None
        pos = lax.rem(me[AXES[part][2]] + shift * onward + N4, N4)
        return ((pos, None, k), (k, None, pos), (k, pos, None))[part]

    def rows_of(item):
        return N4 if item[0] == N3 else N5

    def z_slices(ref, item, slot):
        part = item[0]
        zd, yd, xd = place(item)
        if part == N3:
            return [(ref.at[zd * N4 + x, 15], buf.at[slot, :, x]) for x in range(N4)]
        if part == 2:
            return [(ref.at[pl.ds(zd * N4, N4), pl.ds(ROW0[part], N5), yd], buf.at[slot])]
        return [(ref.at[zd * N4 + xd, ROW0[part] + r], buf.at[slot, :, r]) for r in range(N5)]

    def g_slices(item, slot):
        part, _, k, src = item
        ref = srcs[src]
        if part == N3:
            return [(ref.at[k, :, x], gbuf.at[slot, :, x]) for x in range(N4)]
        return [(ref.at[:, k] if part == 0 else ref.at[k], gbuf.at[slot])]

    def start_in(i):
        slot = i % SLOTS
        for src, dst in z_slices(z_ref, items[i], slot):
            pltpu.make_async_copy(src, dst, in_sem.at[slot, 0]).start()
        for src, dst in g_slices(items[i], slot):
            pltpu.make_async_copy(src, dst, in_sem.at[slot, 1]).start()

    def wait_in(i):
        slot = i % SLOTS
        n = rows_of(items[i])
        zb, gb = buf.at[slot, :, pl.ds(0, n)], gbuf.at[slot, :, pl.ds(0, n)]
        pltpu.make_async_copy(zb, zb, in_sem.at[slot, 0]).wait()
        pltpu.make_async_copy(gb, gb, in_sem.at[slot, 1]).wait()

    def start_out(i):
        slot = i % SLOTS
        for dst, src in z_slices(out_ref, items[i], slot):
            pltpu.make_async_copy(src, dst, out_sem.at[slot]).start()

    def wait_out(i):
        slot = i % SLOTS
        zb = buf.at[slot, :, pl.ds(0, rows_of(items[i]))]
        pltpu.make_async_copy(zb, zb, out_sem.at[slot]).wait()

    def compute(i):
        slot = i % SLOTS
        item = items[i]
        part = item[0]
        zd, yd, xd = place(item)

        offs = tuple(x * N16 for x in range(N4)) if part == N3 else tuple(range(N5))

        def body(q, _):
            lane, yq = zd * N64, q
            if part == N3:
                lane = lane + 15
            elif part == 2:
                lane, yq = lane + q * N16 + ROW0[part], yd
            else:
                lane = lane + xd * N16 + ROW0[part]
            inv = inv_ref[lane // N128, pl.ds(pl.multiple_of(yq * N128, N128), N128), :]
            inv = pltpu.roll(inv, lax.rem(N256 - lane, N128), 1)
            for r, off in enumerate(offs):
                seg = gbuf[slot, q, r].astype(jnp.float32)
                buf[slot, q, r] = buf[slot, q, r] + (seg + bias) * inv[:, off:off + 1]
            return 0

        lax.fori_loop(0, N4, body, 0)

    n = len(items)
    for i in range(min(AHEAD, n)):
        start_in(i)
    for i in range(n):
        j = i + AHEAD
        if j < n:
            if j >= SLOTS:
                wait_out(j - SLOTS)
            start_in(j)
        wait_in(i)
        compute(i)
        start_out(i)
    for i in range(max(0, n - SLOTS), n):
        wait_out(i)


def update(name, items, pair5, inv2, bias, srcs, prev):
    any_spec = pl.BlockSpec(memory_space=pl.ANY)
    vmem_spec = pl.BlockSpec(memory_space=pltpu.VMEM)
    args = [pair5, inv2, bias] + srcs + ([] if prev is None else [prev])
    blocks = len(items) * N16
    return pl.pallas_call(
        functools.partial(update_kernel, items, len(srcs), len(args) - N3 - len(srcs)),
        in_specs=[any_spec, vmem_spec, vmem_spec] + [any_spec] * (len(args) - N3),
        out_specs=any_spec,
        out_shape=jax.ShapeDtypeStruct(pair5.shape, jnp.float32),
        scratch_shapes=[pltpu.VMEM((SLOTS, N4, N5, N128, N128), jnp.float32), pltpu.VMEM((SLOTS, N4, N5, N128, N128), jnp.bfloat16), pltpu.SemaphoreType.DMA((SLOTS, 2)), pltpu.SemaphoreType.DMA((SLOTS,))],
        input_output_aliases={} if prev is None else {len(args) - 1: 0},
        cost_estimate=pl.CostEstimate(flops=blocks * 40_000_000, bytes_accessed=blocks * 163840, transcendentals=0),
        name=name,
    )(*args)


def ring(axis, step, mirror):
    out = []
    for i in range(N64):
        pos = i // STRIDES[axis] % N4
        for core in range(2):
            to = i + ((pos + step * (1 - 2 * core * mirror)) % N4 - pos) * STRIDES[axis]
            out.append((2 * i + core, 2 * to + core))
    return out


def gather_and_update(tile, pair_rows, inv2, bias):
    own, near, last_row = gather(tile)
    pair5 = pair_rows.reshape(N16, N16, N4, N128, N128)
    send = lambda x, p, step: lax.ppermute(x, ('seq', 'dap'), ring(AXES[p][2], step, 1))
    items = lambda shift, base: [(p, shift, k, base + p) for p in range(N3) for k in range(N4)]
    ahead = [send(own[p], p, -1) for p in range(N3)]
    first = [(N3, 0, k, N3) for k in range(N4)] + items(0, 0)
    out = update('update_own', first, pair5, inv2, bias, list(own) + [last_row], None)
    near, out = lax.optimization_barrier((near, out))
    far = [send(near[p], p, 1) for p in range(N3)]
    out = update('update_behind', items(-1, 0), pair5, inv2, bias, list(near), out)
    out = update('update_ahead', items(1, 0), pair5, inv2, bias, ahead, out)
    out = update('update_far', items(2, 0), pair5, inv2, bias, far, out)
    return out.reshape(pair_rows.shape)


def solution(mesh):
    rep = P()
    in_specs = (P(('data', 'seq'), 'dap', None), P('data', None), P(('data', 'dap'), None, None)) + (rep,) * N8
    out_specs = (P(('data', 'dap'), None, None), P(('data', 'seq', 'dap'), None, None))

    def local_fn(msa, mask, pair_rows, ln_gamma, ln_beta, w_left, b_left, w_right, b_right, w_out, b_out):
        dap_idx = lax.axis_index('dap')
        msa_t = jnp.swapaxes(msa, 1, 2)
        rows = jnp.stack([ln_gamma, ln_beta, jnp.concatenate([b_left, b_right])]).astype(jnp.float32)
        vecs = jnp.pad(rows, ((0, N5), (0, N64)))
        a_loc, b_loc = project(msa_t, mask, vecs, w_left.T, w_right.T)
        a_full, b_full, m_full = exchange(a_loc, b_loc, msa_t)
        msa_out = jnp.swapaxes(m_full, 1, 2)
        w2 = w_out.reshape(N32, N32, N128).transpose(2, 1, 0).reshape(N128, 1024)
        terms = pair_partial(a_full, b_full, w2)
        move = lambda v, step, mirror: lax.ppermute(v, ('seq', 'dap'), ring(2, step, mirror))
        relay = move(terms[2], 1, 1)
        after, before = move(terms[1], 1, 0), move(terms[N3], -1, 0)
        parts = [terms[0], after, before, move(relay, 1, 1)]
        total = sum(v.astype(jnp.float32) for v in parts).astype(jnp.bfloat16)

        mask_bf16 = mask.astype(jnp.bfloat16)
        mask_rows = lax.dynamic_slice_in_dim(mask_bf16, dap_idx * N256, N256, axis=1)
        count_t = jnp.einsum('sj,sti->tji', mask_bf16, mask_rows.reshape(2048, 2, N128), preferred_element_type=jnp.float32)
        inv2 = 1.0 / (1e-3 + count_t)
        bias = b_out.astype(jnp.float32).reshape(1, N128)

        total, inv2, bias = lax.optimization_barrier((total, inv2, bias))
        out = gather_and_update(total, pair_rows, inv2, bias)
        return out, msa_out

    return jax.shard_map(local_fn, mesh=mesh, in_specs=in_specs, out_specs=out_specs, check_vma=False)
```
